256 devices in a mesh: sph: 32 (over x, z), ang: 8 (over y, core).
Axes of the slice: x: 4, y: 4, z: 8, core: 2. Of those that a mesh axis runs over, the one named last changes fastest.
Arguments:
- coefficients: bfloat16 [2048, 240, 1024], P(('sph', 'ang')), may hold values from -0.039794922 to 0.039794922
- positions: int32 [2048, 3], P(('sph', 'ang')), may hold values from 0 to 7
- shift_tables: bfloat16 [3, 8, 480, 240], replicated, may hold values from -1.3 to 1.3
- absorb_weight: float32 [2048, 240], P(('sph', 'ang')), may hold values from 0.02 to 0.9, as said below
- incident: float32 [240, 1024], replicated, may hold values from -1.6 to 1.6
- detector: float32 [128, 64], P('sph'), may hold values from 0.002 to 0.18, as said below
Outputs:
- amplitude: float32 [2, 2, 128, 64, 512], P(None, None, 'sph', 'ang')
- cross_sections: float32 [3, 512], P(None, 'ang')
The draws below stay inside these ranges and needn't reach their ends.
Inputs may be any that keep to these rules, and one draw needn't show every extreme that they name: `absorb_weight`: Positive. `detector`: Positive.
All inputs are finite; a program needn't handle non-finite values.
Results may differ from the reference program's by a relative error of at most 0.0003.
The reference program's roundings to bfloat16 on the way (of `first` and `second`) count: a program that leaves them out, or rounds other values in their place, can miss the bound.
Values sent between devices are 32-bit elements; how exact they have to be, the bound alone decides.
No kernel may reach another device: no remote copies, remote signals or barrier semaphores. Data moves between devices by JAX's collectives and lax.ppermute only.
A program may use at most 128 MiB of HBM per device.

```python
import math
import jax
import jax.numpy as jnp
from jax import lax

ORDER = 10
NCOEF = 240
AZIM = 64
GRID = 8
SPH_DEV = 8
FIELDS = 512
SPHERES = 2048
POLAR = 128


def draw_shift_tables(key, part):
    diag_key = jax.random.fold_in(key, 11)
    noise_key = jax.random.fold_in(key, 12)
    diagonal = jax.random.uniform(diag_key, (3, GRID, NCOEF), jnp.float32, 0.7, 1.3)
    spread = 0.3 / math.sqrt(NCOEF)
    noise = jnp.clip(jax.random.normal(noise_key, (3, GRID, 2 * NCOEF, NCOEF), jnp.float32), -4.0, 4.0) * spread
    identity = jnp.eye(NCOEF, dtype=jnp.float32)
    real_block = noise[:, :, :NCOEF, :] * (1.0 - identity) + diagonal[:, :, :, None] * identity
    return jnp.concatenate([real_block, noise[:, :, NCOEF:, :]], axis=2).astype(jnp.bfloat16)


def draw_absorb_weight(key, part):
    rate = jnp.exp(jax.random.uniform(jax.random.fold_in(key, 21), (SPHERES, NCOEF), jnp.float32, math.log(0.02), math.log(0.1)))
    ramp = 1.0 + 2.0 * jnp.arange(SPHERES, dtype=jnp.float32)[:, None] / max(SPHERES - 1, 1)
    return rate * ramp


def draw_detector(key, part):
    rate = jnp.exp(jax.random.uniform(jax.random.fold_in(key, 31), (POLAR, AZIM), jnp.float32, math.log(0.002), math.log(0.02)))
    ramp = 1.0 + 2.0 * jnp.arange(POLAR, dtype=jnp.float32)[:, None] / max(POLAR - 1, 1)
    return rate * ramp


def touch_ends(values, key, smallest, largest):
    extent = values.shape
    place = [jax.random.randint(jax.random.fold_in(key, axis), (), 0, extent[axis]) for axis in range(len(extent))]
    values = values.at[tuple(place)].set(smallest)
    longest = extent.index(max(extent))
    place[longest] = (place[longest] + 1) % extent[longest]
    return values.at[tuple(place)].set(largest)


def shard_levels(key, shape, pieces, smallest, high):
    def one(axis_at, shards_of):
        draws = jax.random.uniform(jax.random.fold_in(jax.random.fold_in(key, 6), axis_at), (shards_of,), jnp.float32, smallest / len(pieces), high / len(pieces))
        return jnp.repeat(jnp.exp(draws), shape[axis_at] // shards_of).reshape((-1,) + (1,) * (len(shape) - axis_at - 1))

    factor_of = one(*pieces[0])
    for cut in pieces[1:]:
        factor_of = factor_of * one(*cut)
    return factor_of


def bell_draw(rng, dims, scale, bound, shards=(), kind=jnp.bfloat16):
    loudness = shard_levels(rng, dims, shards, -0.22, 0.18) if shards else 1.0
    values = jax.random.normal(rng, dims, jnp.float32) * scale * loudness
    return jnp.minimum(jnp.maximum(values, -bound), bound).astype(kind)


def setup_inputs(seed: int = 0) -> dict:
    key_of = jax.random.split(jax.random.key(seed), 7)
    coefficients = bell_draw(key_of[0], (SPHERES, NCOEF, 2 * FIELDS), 0.005, 0.039794922, ((0, 256),))
    positions = touch_ends(jax.random.randint(key_of[1], (SPHERES, 3), 0, GRID), jax.random.fold_in(key_of[1], 1), 0, GRID - 1).astype(jnp.int32)
    shift_tables = draw_shift_tables(jax.random.fold_in(key_of[6], 71), 0)
    absorb_weight = draw_absorb_weight(jax.random.fold_in(key_of[6], 71), 0)
    incident = bell_draw(key_of[4], (NCOEF, 2 * FIELDS), 0.2, 1.6, (), jnp.float32)
    detector = draw_detector(jax.random.fold_in(key_of[6], 71), 0)
    return dict(coefficients=coefficients, positions=positions, shift_tables=shift_tables, absorb_weight=absorb_weight, incident=incident, detector=detector)


def legendre_table(cos_theta, sine_theta, order):
    values = {}
    values[0, 0] = jnp.zeros_like(cos_theta) + 1.0 / math.sqrt(4.0 * math.pi)
    for azim_order in range(order + 1):
        if azim_order > 0:
            factor = -math.sqrt((2.0 * azim_order + 1.0) / (2.0 * azim_order))
            values[azim_order, azim_order] = factor * sine_theta * values[azim_order - 1, azim_order - 1]
        if azim_order + 1 <= order:
            values[azim_order + 1, azim_order] = math.sqrt(2.0 * azim_order + 3.0) * cos_theta * values[azim_order, azim_order]
        for degree in range(azim_order + 2, order + 1):
            upper_coef = math.sqrt((4.0 * degree * degree - 1.0) / (degree * degree - azim_order * azim_order))
            lower_coef = math.sqrt(((degree - 1.0) * (degree - 1.0) - azim_order * azim_order) / (4.0 * (degree - 1.0) * (degree - 1.0) - 1.0))
            values[degree, azim_order] = upper_coef * (cos_theta * values[degree - 1, azim_order] - lower_coef * values[degree - 2, azim_order])
    return values

def angular_basis(polar_index, azim_index, polar_total, azim_total, order):
    theta = (polar_index.astype(jnp.float32) + 0.5) * (math.pi / polar_total)
    azimuth = azim_index.astype(jnp.float32) * (2.0 * math.pi / azim_total)
    cos_theta = jnp.cos(theta)
    sine_theta = jnp.sin(theta)
    legendre_values = legendre_table(cos_theta, sine_theta, order)
    pi_terms = []
    tau_terms = []
    orders_list = []
    phase_real = []
    phase_imag = []
    unit_powers = [(1.0, 0.0), (0.0, -1.0), (-1.0, 0.0), (0.0, 1.0)]
    for degree in range(1, order + 1):
        norm_factor = 1.0 / math.sqrt(degree * (degree + 1.0))
        power_real, power_imag = unit_powers[(degree + 1) % 4]
        for azim_order in range(-degree, degree + 1):
            size_m = abs(azim_order)
            current = legendre_values[degree, size_m]
            if degree - 1 >= size_m:
                previous = legendre_values[degree - 1, size_m]
            else:
                previous = jnp.zeros_like(current)
            link = math.sqrt((2.0 * degree + 1.0) * (degree * degree - azim_order * azim_order) / (2.0 * degree - 1.0))
            pi_terms.append(azim_order * current / sine_theta)
            tau_terms.append((degree * cos_theta * current - link * previous) / sine_theta)
            orders_list.append(float(azim_order))
            phase_real.append(power_real * norm_factor)
            phase_imag.append(power_imag * norm_factor)
    pi_block = jnp.stack(pi_terms, axis=1)[:, None, :]
    tau_block = jnp.stack(tau_terms, axis=1)[:, None, :]
    orders_row = jnp.array(orders_list, dtype=jnp.float32)
    angle_table = azimuth[:, None] * orders_row[None, :]
    cos_table = jnp.cos(angle_table)
    sin_table = jnp.sin(angle_table)
    scale_real = jnp.array(phase_real, dtype=jnp.float32)[None, :]
    scale_imag = jnp.array(phase_imag, dtype=jnp.float32)[None, :]
    wave_real = (scale_real * cos_table - scale_imag * sin_table)[None, :, :]
    wave_imag = (scale_real * sin_table + scale_imag * cos_table)[None, :, :]
    theta_real = jnp.concatenate([-pi_block * wave_imag, tau_block * wave_real], axis=-1)
    theta_imag = jnp.concatenate([pi_block * wave_real, tau_block * wave_imag], axis=-1)
    phi_real = jnp.concatenate([-tau_block * wave_real, -pi_block * wave_imag], axis=-1)
    phi_imag = jnp.concatenate([-tau_block * wave_imag, pi_block * wave_real], axis=-1)
    real_part = jnp.stack([theta_real, phi_real])
    imag_part = jnp.stack([theta_imag, phi_imag])
    return (real_part, imag_part, sine_theta)

def evaluate_far(real_part, imag_part, anchor):
    half = anchor.shape[1] // 2
    first = jnp.einsum('cikp,pf->cikf', real_part, anchor, precision=lax.Precision.HIGHEST)
    second = jnp.einsum('cikp,pf->cikf', imag_part, anchor, precision=lax.Precision.HIGHEST)
    real_out = first[..., :half] - second[..., half:]
    imag_out = first[..., half:] + second[..., :half]
    return jnp.stack([real_out, imag_out], axis=1)

def rotate_step(matrix, vector):
    product = jnp.einsum('sap,spf->saf', matrix.astype(jnp.float32), vector.astype(jnp.float32))
    half_rows = matrix.shape[2]
    half_cols = vector.shape[2] // 2
    real_out = product[:, :half_rows, :half_cols] - product[:, half_rows:, half_cols:]
    imag_out = product[:, half_rows:, :half_cols] + product[:, :half_rows, half_cols:]
    return jnp.concatenate([real_out, imag_out], axis=2)

def reference(coefficients, positions, shift_tables, absorb_weight, incident, detector):
    blocks = coefficients.shape[0] // SPH_DEV
    coef_blocks = coefficients.reshape(blocks, SPH_DEV, NCOEF, 2 * FIELDS)
    cell_blocks = positions.reshape(blocks, SPH_DEV, 3)
    weight_blocks = absorb_weight.reshape(blocks, SPH_DEV, NCOEF)

    def accumulate(carry, inputs):
        anchor_acc, absorbed_acc = carry
        block_coef, block_cells, block_weight = inputs
        along_z = jnp.take(shift_tables[2], block_cells[:, 2], axis=0)
        along_y = jnp.take(shift_tables[1], block_cells[:, 1], axis=0)
        along_x = jnp.take(shift_tables[0], block_cells[:, 0], axis=0)
        first = rotate_step(along_z, block_coef).astype(jnp.bfloat16)
        second = rotate_step(along_y, first).astype(jnp.bfloat16)
        moved = rotate_step(along_x, second)
        widened = block_coef.astype(jnp.float32)
        squares = widened * widened
        energy = squares[:, :, :FIELDS] + squares[:, :, FIELDS:]
        absorbed_acc = absorbed_acc + jnp.einsum('sp,spf->f', block_weight, energy)
        return ((anchor_acc + lax.optimization_barrier(jnp.sum(moved, axis=0)), absorbed_acc), None)
    start = (jnp.zeros((NCOEF, 2 * FIELDS), jnp.float32), jnp.zeros((FIELDS,), jnp.float32))
    (anchor, absorbed), ignored = lax.scan(accumulate, start, (coef_blocks, cell_blocks, weight_blocks))
    extinction = lax.optimization_barrier(jnp.sum(incident[:, :FIELDS] * anchor[:, :FIELDS] + incident[:, FIELDS:] * anchor[:, FIELDS:], axis=0))
    real_part, imag_part, sine_theta = angular_basis(jnp.arange(POLAR), jnp.arange(AZIM), POLAR, AZIM, ORDER)
    amplitude = evaluate_far(real_part, imag_part, anchor)
    weight = detector * sine_theta[:, None] * (2.0 * math.pi * math.pi / (POLAR * AZIM))
    collected = jnp.einsum('crikf,ik->f', amplitude * amplitude, weight)
    cross_sections = jnp.stack([extinction, absorbed, collected])
    return (amplitude, cross_sections)
```

```python
import functools
import math

import jax
import jax.numpy as jnp
from jax import lax
from jax.experimental import pallas as pl
from jax.experimental.pallas import tpu as pltpu
from jax.sharding import Mesh
from jax.sharding import PartitionSpec as P

ORDER = 10
AZIM = 64
POL_DEV = 4
SPH = ("sph_0", "sph_1")
ANG = ("ang_0", "ang_1")
SPH_ANG = ("sph_0", "sph_1", "ang_0", "ang_1")


def cut_along(shard, dim, size):
    shape = shard.shape
    parts = shard.reshape(*shape[:dim], size, shape[dim] // size, *shape[dim + 1 :])
    return jnp.moveaxis(parts, dim, 0)


def sum_at_owner(shard, axis, dim):
    parts = cut_along(shard, dim, lax.axis_size(axis))
    arrived = lax.all_to_all(parts, axis, split_axis=0, concat_axis=0, tiled=True)
    return arrived.sum(axis=0)


def summed_rows(shard, axes, dim):
    far, near = axes
    parts = cut_along(shard, dim, lax.axis_size(far))
    nearer = sum_at_owner(parts, near, dim + 1)
    arrived = lax.all_to_all(nearer, far, split_axis=0, concat_axis=0, tiled=True)
    return arrived.sum(axis=0)


def rows_for(lines, size):
    spare = -len(lines) % size
    return jnp.pad(lines, [(0, spare)] + [(0, 0)] * (lines.ndim - 1))


def from_everyone(shard, axis):
    size = lax.axis_size(axis)
    return lax.all_to_all(
        jnp.broadcast_to(shard[None], (size, *shard.shape)), axis, 0, 0, tiled=True
    )


def laid_out(parts, dim):
    shape = list(parts.shape[1:])
    shape[dim] *= parts.shape[0]
    return jnp.moveaxis(parts, 0, dim).reshape(shape)


def gathered_by_axis(shard, axes, dim):
    far, near = axes
    leading = from_everyone(shard, far)
    parts = jnp.swapaxes(from_everyone(leading, near), 0, 1)
    return laid_out(parts.reshape(-1, *shard.shape), dim)


def total_of(shard, axes):
    own = summed_rows(rows_for(shard, lax.axis_size(axes[0]) * lax.axis_size(axes[1])), axes, 0)
    whole = gathered_by_axis(own, axes, 0)
    return whole[: len(shard)].reshape(shard.shape)


def packed_total(arrays, axis):
    ravelled, at, done = (jnp.concatenate([a.reshape(-1) for a in arrays]), 0, [])
    so_far = total_of(ravelled, axis)
    for a in arrays:
        done.append(so_far[at : at + a.size].reshape(a.shape))
        at += a.size
    return tuple(done)


def over_copies(shard, axis):
    everything = from_everyone(shard, axis)
    return jnp.sum(everything, axis=0)


def legendre_table(cos_theta, sine_theta, order):
    values = {}
    values[0, 0] = jnp.zeros_like(cos_theta) + 1.0 / math.sqrt(4.0 * math.pi)
    for azim_order in range(order + 1):
        if azim_order > 0:
            factor = -math.sqrt((2.0 * azim_order + 1.0) / (2.0 * azim_order))
            values[azim_order, azim_order] = (
                factor * sine_theta * values[azim_order - 1, azim_order - 1]
            )
        if azim_order + 1 <= order:
            values[azim_order + 1, azim_order] = (
                math.sqrt(2.0 * azim_order + 3.0) * cos_theta * values[azim_order, azim_order]
            )
        for degree in range(azim_order + 2, order + 1):
            upper_coef = math.sqrt(
                (4.0 * degree * degree - 1.0) / (degree * degree - azim_order * azim_order)
            )
            lower_coef = math.sqrt(
                ((degree - 1.0) * (degree - 1.0) - azim_order * azim_order)
                / (4.0 * (degree - 1.0) * (degree - 1.0) - 1.0)
            )
            values[degree, azim_order] = upper_coef * (
                cos_theta * values[degree - 1, azim_order]
                - lower_coef * values[degree - 2, azim_order]
            )
    return values


def angular_basis(polar_index, azim_index, polar_total, azim_total, order):
    theta = (polar_index.astype(jnp.float32) + 0.5) * (math.pi / polar_total)
    azimuth = azim_index.astype(jnp.float32) * (2.0 * math.pi / azim_total)
    cos_theta = jnp.cos(theta)
    sine_theta = jnp.sin(theta)
    legendre_values = legendre_table(cos_theta, sine_theta, order)
    pi_terms = []
    tau_terms = []
    orders_list = []
    phase_real = []
    phase_imag = []
    unit_powers = [(1.0, 0.0), (0.0, -1.0), (-1.0, 0.0), (0.0, 1.0)]
    for degree in range(1, order + 1):
        norm_factor = 1.0 / math.sqrt(degree * (degree + 1.0))
        power_real, power_imag = unit_powers[(degree + 1) % 4]
        for azim_order in range(-degree, degree + 1):
            size_m = abs(azim_order)
            current = legendre_values[degree, size_m]
            if degree - 1 >= size_m:
                previous = legendre_values[degree - 1, size_m]
            else:
                previous = jnp.zeros_like(current)
            link = math.sqrt(
                (2.0 * degree + 1.0)
                * (degree * degree - azim_order * azim_order)
                / (2.0 * degree - 1.0)
            )
            pi_terms.append(azim_order * current / sine_theta)
            tau_terms.append((degree * cos_theta * current - link * previous) / sine_theta)
            orders_list.append(float(azim_order))
            phase_real.append(power_real * norm_factor)
            phase_imag.append(power_imag * norm_factor)
    pi_block = jnp.stack(pi_terms, axis=1)[:, None, :]
    tau_block = jnp.stack(tau_terms, axis=1)[:, None, :]
    orders_row = jnp.array(orders_list, dtype=jnp.float32)
    angle_table = azimuth[:, None] * orders_row[None, :]
    cos_table = jnp.cos(angle_table)
    sin_table = jnp.sin(angle_table)
    scale_real = jnp.array(phase_real, dtype=jnp.float32)[None, :]
    scale_imag = jnp.array(phase_imag, dtype=jnp.float32)[None, :]
    wave_real = (scale_real * cos_table - scale_imag * sin_table)[None, :, :]
    wave_imag = (scale_real * sin_table + scale_imag * cos_table)[None, :, :]
    theta_real = jnp.concatenate([-pi_block * wave_imag, tau_block * wave_real], axis=-1)
    theta_imag = jnp.concatenate([pi_block * wave_real, tau_block * wave_imag], axis=-1)
    phi_real = jnp.concatenate([-tau_block * wave_real, -pi_block * wave_imag], axis=-1)
    phi_imag = jnp.concatenate([-tau_block * wave_imag, pi_block * wave_real], axis=-1)
    real_part = jnp.stack([theta_real, phi_real])
    imag_part = jnp.stack([theta_imag, phi_imag])
    return (real_part, imag_part, sine_theta)


def evaluate_far(real_part, imag_part, anchor):
    half = anchor.shape[1] // 2
    first = jnp.einsum("cikp,pf->cikf", real_part, anchor, precision=lax.Precision.HIGHEST)
    second = jnp.einsum("cikp,pf->cikf", imag_part, anchor, precision=lax.Precision.HIGHEST)
    real_out = first[..., :half] - second[..., half:]
    imag_out = first[..., half:] + second[..., :half]
    return jnp.stack([real_out, imag_out], axis=1)


COEFS = 240
FIELDS = 512
PADDED = 512


def move_kernel(unroll, cells_ref, coef_ref, *refs):
    tables = refs[: 3 * unroll]
    weight_ref, moved_ref, absorbed_ref, left, right = refs[3 * unroll :]
    step = pl.program_id(0)

    @pl.when(step == 0)
    def _():
        moved_ref[...] = jnp.zeros_like(moved_ref)
        absorbed_ref[...] = jnp.zeros_like(absorbed_ref)
        left[...] = jnp.zeros_like(left)
        right[...] = jnp.zeros_like(right)

    weights = weight_ref[...].T
    lane = lax.broadcasted_iota(jnp.int32, weights.shape, 1)
    for s in range(unroll):
        real, imag = coef_ref[s, :, :FIELDS], coef_ref[s, :, FIELDS:]
        right[s, :COEFS] = real
        right[s, 256 : 256 + COEFS] = imag
        column = jnp.sum(
            jnp.where(lane == step * unroll + s, weights, 0.0), axis=1, keepdims=True
        )
        real, imag = real.astype(jnp.float32), imag.astype(jnp.float32)
        energy = (real * real + imag * imag) * column
        absorbed_ref[...] += jnp.sum(energy.reshape(COEFS // 8, 8, FIELDS), axis=0)
    for stage in range(3):
        for s in range(unroll):
            table = tables[stage * unroll + s]
            left[s, stage, :, :COEFS] = table[0, 0]
            left[s, stage, :COEFS, 256 : 256 + COEFS] = -table[0, 0, COEFS:]
            left[s, stage, COEFS:, 256 : 256 + COEFS] = table[0, 0, :COEFS]
            product = jnp.dot(left[s, stage], right[s], preferred_element_type=jnp.float32)
            if stage < 2:
                product = product.astype(jnp.bfloat16)
                right[s, :COEFS] = product[:COEFS]
                right[s, 256 : 256 + COEFS] = product[COEFS:]
            else:
                moved_ref[...] += product


def moved_sum(coefficients, positions, shift_tables, absorb_weight, unroll=2):
    spheres = coefficients.shape[0]

    def table_of(axis, s):
        return pl.BlockSpec(
            (1, 1, 2 * COEFS, COEFS),
            lambda j, cells: (axis, cells[(j * unroll + s) * 3 + axis], 0, 0),
        )

    return pl.pallas_call(
        functools.partial(move_kernel, unroll),
        grid_spec=pltpu.PrefetchScalarGridSpec(
            num_scalar_prefetch=1,
            grid=(spheres // unroll,),
            in_specs=[pl.BlockSpec((unroll, COEFS, 2 * FIELDS), lambda j, cells: (j, 0, 0))]
            + [table_of(axis, s) for axis in (2, 1, 0) for s in range(unroll)]
            + [pl.BlockSpec((spheres, COEFS), lambda j, cells: (0, 0))],
            out_specs=[
                pl.BlockSpec((2 * COEFS, FIELDS), lambda j, cells: (0, 0)),
                pl.BlockSpec((8, FIELDS), lambda j, cells: (0, 0)),
            ],
            scratch_shapes=[
                pltpu.VMEM((unroll, 3, 2 * COEFS, PADDED), jnp.bfloat16),
                pltpu.VMEM((unroll, PADDED, FIELDS), jnp.bfloat16),
            ],
        ),
        out_shape=[
            jax.ShapeDtypeStruct((2 * COEFS, FIELDS), jnp.float32),
            jax.ShapeDtypeStruct((8, FIELDS), jnp.float32),
        ],
        compiler_params=pltpu.CompilerParams(dimension_semantics=("arbitrary",)),
        cost_estimate=pl.CostEstimate(
            flops=6_000_000_000, bytes_accessed=10_000_000, transcendentals=0
        ),
        name="move",
    )(positions.reshape(-1), coefficients, *([shift_tables] * (3 * unroll)), absorb_weight)


def shards(coefficients, positions, shift_tables, absorb_weight, incident, detector):
    fields = coefficients.shape[2] // 2
    coef_count = coefficients.shape[1]
    moved, absorbed = moved_sum(coefficients, positions, shift_tables, absorb_weight)
    absorbed = jnp.sum(absorbed, axis=0)
    partial_value = jnp.concatenate([moved[:coef_count], moved[coef_count:]], axis=1)
    extinction = jnp.sum(
        incident[:, :fields] * partial_value[:, :fields]
        + incident[:, fields:] * partial_value[:, fields:],
        axis=0,
    )
    local_stats = jnp.stack([extinction, absorbed])
    partial_split = partial_value.reshape(coef_count, 2, fields)
    polar_total = POL_DEV * lax.axis_size(SPH)
    polar_index = lax.axis_index(SPH) * POL_DEV + jnp.arange(POL_DEV)
    groups = lax.axis_size(ANG)
    share = fields // groups
    solid_angle = 2.0 * math.pi * math.pi / (polar_total * AZIM)
    anchor_split, stats = packed_total(
        (partial_split, local_stats), (("sph_0", "sph_1"), ("ang_0", "ang_1"))
    )
    azim_share = AZIM // groups
    azim_start = lax.axis_index(ANG) * azim_share
    azim_index = azim_start + jnp.arange(azim_share)
    real_part, imag_part, sine_theta = angular_basis(
        polar_index, azim_index, polar_total, AZIM, ORDER
    )
    amplitude = evaluate_far(real_part, imag_part, anchor_split.reshape(coef_count, 2 * fields))
    local_detector = lax.dynamic_slice_in_dim(detector, azim_start, azim_share, 1)
    weight = local_detector * sine_theta[:, None] * solid_angle
    power = jnp.einsum("crikf,ik->f", amplitude * amplitude, weight)
    collected = sum_at_owner(power, ANG, 0)
    collected = over_copies(collected, SPH)
    own_stats = lax.dynamic_slice_in_dim(stats, lax.axis_index(ANG) * share, share, 1)
    cross_sections = jnp.concatenate([own_stats, collected[None, :]], axis=0)
    return (amplitude, cross_sections)


def solution(mesh):
    torus = Mesh(mesh.devices.reshape(4, 8, 4, 2), ("sph_0", "sph_1", "ang_0", "ang_1"))
    in_specs = (P(SPH_ANG, None, None), P(SPH_ANG, None), P(), P(SPH_ANG, None), P(), P(SPH, None))
    out_specs = (P(None, None, SPH, ANG, None), P(None, ANG))
    return jax.shard_map(
        shards, mesh=torus, in_specs=in_specs, out_specs=out_specs, check_vma=False
    )
```

```python
import functools
import math

import jax
import jax.numpy as jnp
import numpy as np
from jax import lax
from jax.experimental import pallas as pl
from jax.experimental.pallas import tpu as pltpu
from jax.sharding import Mesh
from jax.sharding import PartitionSpec as P

ORDER = 10
AZIM = 64
POLAR = 128
COEFS = 240
HALF = 120
FIELDS = 512
ROWS = 256
CHUNK = 32
LANES = 128
SPH_ANG = ("sph_0", "sph_1", "ang_0", "ang_1")
SPH = ("sph_0", "sph_1")
ANG = ("ang_0", "ang_1")
PLANE = ("ang_0", "sph_0")
LINE = "sph_1"
PAIR = "ang_1"
F32 = jnp.float32
BF16 = jnp.bfloat16


def index_tables():
    degree, order = np.zeros(LANES), np.zeros(LANES)
    for n in range(1, ORDER + 1):
        for m in range(-n, n + 1):
            degree[n * n - 1 + n + m] = n
            order[n * n - 1 + n + m] = m
    size = np.abs(order)
    used = degree > 0
    rise, fall = np.zeros((ORDER + 1, LANES)), np.zeros((ORDER + 1, LANES))
    for t in range(1, ORDER + 1):
        on = used & (size < t) & (t <= degree)
        s = size[on]
        rise[t, on] = np.sqrt((4.0 * t * t - 1.0) / (t * t - s * s))
        if t > 1:
            fall[t, on] = np.sqrt(((t - 1.0) ** 2 - s * s) / (4.0 * (t - 1.0) ** 2 - 1.0))
    link = np.sqrt((2 * degree + 1) * (degree**2 - order**2) / np.maximum(2 * degree - 1, 1)) * used
    norm = used / np.sqrt(np.maximum(degree * (degree + 1.0), 1.0))
    unit = np.array([1.0, -1.0j, -1.0, 1.0j])[(degree.astype(int) + 1) % 4] * norm
    return degree, order, size, rise, fall, link, unit


def radial(cos_theta, sine_theta):
    degree, order, size, rise, fall, link, _ = index_tables()
    row = lambda v: jnp.asarray(np.asarray(v, np.float32)[None, :])
    current = jnp.full((cos_theta.shape[0], LANES), 1.0 / math.sqrt(4.0 * math.pi), F32)
    for t in range(1, ORDER + 1):
        factor = -math.sqrt((2.0 * t + 1.0) / (2.0 * t))
        current = jnp.where(row(size) >= t, factor * sine_theta * current, current)
    previous = jnp.zeros_like(current)
    for t in range(1, ORDER + 1):
        following = row(rise[t]) * (cos_theta * current - row(fall[t]) * previous)
        on = row(rise[t]) > 0
        previous, current = jnp.where(on, current, previous), jnp.where(on, following, current)
    pi_term = row(order) * current / sine_theta
    tau_term = (row(degree) * cos_theta * current - row(link) * previous) / sine_theta
    return jnp.stack([tau_term + pi_term, tau_term - pi_term])


def halves(value):
    high = value.astype(BF16)
    return high, (value - high.astype(F32)).astype(BF16)


def swap_chunks(blocks):
    group = lax.broadcasted_iota(jnp.int32, blocks[0].shape, 1) // CHUNK
    out = []
    for x in range(4):
        mixed = None
        for g in range(4):
            shift = (g - x) * CHUNK % LANES
            piece = pltpu.roll(blocks[g], shift, 1) if shift else blocks[g]
            mixed = piece if mixed is None else jnp.where(group == g, piece, mixed)
        out.append(mixed)
    return out


def call(body, outs, ins, name, flops=1, limit=16, **kw):
    size = sum(math.prod(a.shape) * a.dtype.itemsize for a in list(outs) + list(ins))
    return pl.pallas_call(
        body,
        out_shape=[jax.ShapeDtypeStruct(o.shape, o.dtype) for o in outs],
        compiler_params=pltpu.CompilerParams(vmem_limit_bytes=limit * 1024 * 1024),
        cost_estimate=pl.CostEstimate(flops=flops, bytes_accessed=size, transcendentals=0),
        name=name,
        **kw,
    )(*ins)


def struct(shape, dtype=F32):
    return jax.ShapeDtypeStruct(shape, dtype)


def move_kernel(
    unroll, scalar_ref, coef_hbm, table_hbm, weight_ref, mine_ref, theirs_ref,
    coef, table, total, absorbed, right, sems,
):
    spheres = coef.shape[0]
    groups = spheres // unroll

    def coef_copy(j):
        return pltpu.make_async_copy(coef_hbm.at[j], coef.at[j], sems.at[3, j])

    def table_copy(j, stage):
        axis = 2 - stage
        cell = scalar_ref[1 + 3 * j + axis]
        return pltpu.make_async_copy(
            table_hbm.at[axis, cell], table.at[stage, j], sems.at[stage, j]
        )

    def fetches(group):
        own = range(group * unroll, (group + 1) * unroll)
        first = [copy for j in own for copy in (coef_copy(j), table_copy(j, 0))]
        return first, [table_copy(j, stage) for stage in (1, 2) for j in own]

    first, second = fetches(0)
    for copy in first + second:
        copy.start()
    total[...] = jnp.zeros_like(total)
    absorbed[...] = jnp.zeros_like(absorbed)
    weights = weight_ref[...].T
    for group in range(groups):
        if group + 1 < groups:
            ahead = fetches(group + 1)
            for copy in ahead[0] + ahead[1]:
                copy.start()
        for copy in first if group == 0 else first + second:
            copy.wait()
        for s in range(unroll):
            j = group * unroll + s
            real, imag = coef[j, :, :FIELDS].astype(F32), coef[j, :, FIELDS:].astype(F32)
            energy = (real * real + imag * imag) * weights[:, j : j + 1]
            absorbed[...] += jnp.sum(energy.reshape(COEFS // 8, 8, FIELDS), axis=0)
        for stage in range(3):
            if group == 0 and stage == 1:
                for copy in second:
                    copy.wait()
            for s in range(unroll):
                j = group * unroll + s
                matrix = table[stage, j]
                turned = jnp.concatenate([-matrix[COEFS:], matrix[:COEFS]], axis=0)
                if stage == 0:
                    real, imag = coef[j, :, :FIELDS], coef[j, :, FIELDS:]
                else:
                    real, imag = right[s, :COEFS], right[s, ROWS : ROWS + COEFS]
                product = jnp.dot(matrix, real, preferred_element_type=F32) + jnp.dot(
                    turned, imag, preferred_element_type=F32
                )
                if stage < 2:
                    product = product.astype(BF16)
                    right[s, :COEFS] = product[:COEFS]
                    right[s, ROWS : ROWS + COEFS] = product[COEFS:]
                else:
                    total[0, :COEFS] += product[:COEFS]
                    total[1, :COEFS] += product[COEFS:]
        if group + 1 < groups:
            first, second = ahead
    total[0, COEFS : COEFS + 1] = jnp.sum(absorbed[...], axis=0, keepdims=True)
    core = scalar_ref[0]
    mine_ref[...] = total[core]
    theirs_ref[...] = total[1 - core]


def moved_sum(coefficients, positions, shift_tables, absorb_weight, core, unroll=2):
    spheres = coefficients.shape[0]
    scalars = jnp.concatenate([core.reshape(1), positions.reshape(-1)])
    hbm = pl.BlockSpec(memory_space=pltpu.HBM)
    vmem = pl.BlockSpec(memory_space=pltpu.VMEM)
    return pl.pallas_call(
        functools.partial(move_kernel, unroll),
        in_specs=[pl.BlockSpec(memory_space=pltpu.SMEM), hbm, hbm, vmem],
        out_specs=[vmem, vmem],
        scratch_shapes=[
            pltpu.VMEM((spheres, COEFS, 2 * FIELDS), BF16),
            pltpu.VMEM((3, spheres, 2 * COEFS, COEFS), BF16),
            pltpu.VMEM((2, ROWS, FIELDS), F32),
            pltpu.VMEM((8, FIELDS), F32),
            pltpu.VMEM((unroll, 2 * ROWS, FIELDS), BF16),
            pltpu.SemaphoreType.DMA((4, spheres)),
        ],
        out_shape=[struct((ROWS, FIELDS))] * 2,
        compiler_params=pltpu.CompilerParams(vmem_limit_bytes=62 * 1024 * 1024),
        cost_estimate=pl.CostEstimate(
            flops=6_000_000_000, bytes_accessed=10_000_000, transcendentals=0
        ),
        name="move",
    )(scalars, coefficients, shift_tables, absorb_weight)


def pack_kernel(mine_ref, other_ref, detector_ref, out_ref):
    detector = detector_ref[...]
    detector = jnp.concatenate([detector[:, :CHUNK], detector[:, CHUNK:]], axis=0)
    for tile in range(4):
        lanes = slice(tile * LANES, (tile + 1) * LANES)
        blocks = [
            mine_ref[g * 64 : (g + 1) * 64, lanes] + other_ref[g * 64 : (g + 1) * 64, lanes]
            for g in range(4)
        ]
        for x, block in enumerate(swap_chunks(blocks)):
            out_ref[4 * tile + x] = block
            out_ref[4 * tile + x, 56:, 96:] = detector


def plane_kernel(got_ref, out_ref):
    total = got_ref[0]
    for k in range(1, 16):
        total = total + got_ref[k]
    group = lax.broadcasted_iota(jnp.int32, (8, LANES), 1) // CHUNK
    detectors = got_ref[3, 56:]
    for x in range(3):
        detectors = jnp.where(
            group == x, pltpu.roll(got_ref[x, 56:], (x + 1) * CHUNK, 1), detectors
        )
    for k in range(8):
        out_ref[k, :64] = total
        out_ref[k, 64:] = detectors


def basis_kernel(radial_ref, cos_ref, sin_ref, high_ref, low_ref):
    for sign in range(2):
        for trig, ref in enumerate((cos_ref, sin_ref)):
            block = radial_ref[sign][None, :, None, :] * ref[...].reshape(4, 1, 8, LANES)
            high, low = halves(block.reshape(2 * ROWS, LANES))
            lanes = slice((2 * sign + trig) * LANES, (2 * sign + trig + 1) * LANES)
            high_ref[:, lanes] = high
            low_ref[:, lanes] = low


def power_kernel(radial_ref, scaled_ref, line_ref, waves_ref, gap_ref, out_ref):
    gap = gap_ref[...]
    far = jnp.abs(gap)
    far = jnp.concatenate([far, far], axis=1)
    detectors = line_ref[:, 64:].reshape(64, LANES)
    group = lax.broadcasted_iota(jnp.int32, detectors.shape, 1) // CHUNK
    detectors = jnp.concatenate([jnp.where(group == x, detectors, 0.0) for x in range(4)], axis=0)
    spectrum = jnp.dot(
        detectors, waves_ref[...], preferred_element_type=F32, precision=lax.Precision.HIGHEST
    )
    spectrum = spectrum[:, :LANES] + pltpu.roll(spectrum[:, LANES:], 2 * LANES - 4, 0)
    spectrum = jnp.concatenate([spectrum[8 * k : 8 * k + 4] for k in range(32)], axis=0)
    for sign in range(2):
        table = scaled_ref[sign]
        left_high, left_low = halves(radial_ref[sign].T)
        left = jnp.concatenate([left_high, left_high], axis=1)
        total = jnp.zeros((LANES, 2 * LANES), F32)
        for d in range(2 * ORDER + 1):
            right = jnp.concatenate(
                [table * spectrum[:, d : d + 1], table * spectrum[:, 64 + d : 65 + d]], axis=1
            )
            high, low = halves(right)
            product = jnp.dot(
                left, jnp.concatenate([high, low], axis=0), preferred_element_type=F32
            ) + jnp.dot(left_low, high, preferred_element_type=F32)
            total = jnp.where(far == d, product, total)
        out_ref[sign, :, :LANES] = total[:, :LANES]
        out_ref[sign, :, LANES:] = jnp.where(gap < 0, -total[:, LANES:], total[:, LANES:])


def spread_rows(packed):
    parts = [packed] + [pltpu.roll(packed, LANES - g * CHUNK, 1) for g in (1, 2, 3)]
    return jnp.concatenate(parts, axis=0)


def columns(group, pieces):
    out = pieces[0]
    for g in (1, 2, 3):
        out = jnp.where(group == g, pltpu.roll(pieces[g], g * CHUNK, 1), out)
    return out


def far_kernel(
    core_ref, own_ref, other_ref, high_ref, low_ref, form_ref, phase_ref,
    incident_ref, incident_imag_ref, out_ref,
):
    core = core_ref[0]
    own, other = own_ref[...], other_ref[...]
    real = spread_rows(jnp.where(core == 0, own, other))
    imag = spread_rows(jnp.where(core == 0, other, own))
    group = lax.broadcasted_iota(jnp.int32, (HALF, LANES), 1) // CHUNK
    spare = jnp.zeros((8, LANES), F32)
    phase_real, phase_imag = phase_ref[0], phase_ref[1]
    real_1, real_2 = real[:HALF], real[HALF:COEFS]
    imag_1, imag_2 = imag[:HALF], imag[HALF:COEFS]
    rows = []
    collected = jnp.zeros((1, LANES), F32)
    for sign in range(2):
        if sign == 0:
            both = (real_2 - imag_1, imag_2 + real_1)
        else:
            both = (real_2 + imag_1, imag_2 - real_1)
        re = phase_real * both[0] - phase_imag * both[1]
        im = phase_real * both[1] + phase_imag * both[0]
        if sign == 0:
            top = columns(group, (re, im, -im, re))
            low = columns(group, (-im, re, -re, -im))
        else:
            top = columns(group, (re, im, im, -re))
            low = columns(group, (-im, re, re, im))
        rows += [0.5 * top, spare, 0.5 * low, spare]
        pair = jnp.concatenate([jnp.where(group == 0, re, 0.0), spare], axis=0)
        pair_imag = jnp.concatenate([jnp.where(group == 0, im, 0.0), spare], axis=0)
        dot = functools.partial(
            jnp.dot, preferred_element_type=F32, precision=lax.Precision.HIGHEST
        )
        even, odd = form_ref[sign, :, :LANES], form_ref[sign, :, LANES:]
        collected += 0.5 * jnp.sum(
            pair * dot(even, pair)
            + pair_imag * (dot(even, pair_imag) + 2.0 * dot(odd, pair)),
            axis=0,
            keepdims=True,
        )
    high, low = halves(jnp.concatenate(rows, axis=0))
    wide = jnp.dot(
        high_ref[...], jnp.concatenate([high, low], axis=1), preferred_element_type=F32
    )
    result = (
        wide[:, :LANES]
        + wide[:, LANES:]
        + jnp.dot(low_ref[...], high, preferred_element_type=F32)
    )
    extinction = jnp.sum(
        incident_ref[...] * real[:COEFS, :CHUNK] + incident_imag_ref[...] * imag[:COEFS, :CHUNK],
        axis=0,
        keepdims=True,
    )
    stats = jnp.concatenate(
        [
            extinction,
            real[COEFS : COEFS + 1, :CHUNK],
            collected[:, :CHUNK],
            jnp.zeros((1, CHUNK), F32),
        ],
        axis=1,
    )
    stats = jnp.broadcast_to(stats, (8, LANES))
    for k in range(16):
        out_ref[k, :CHUNK] = result[k * CHUNK : (k + 1) * CHUNK]
        out_ref[k, CHUNK:] = stats


def finish_kernel(place_ref, got_ref, amplitude_ref, stats_ref):
    for tile in range(4):
        blocks = [got_ref[4 * tile + x, :CHUNK] for x in range(4)]
        for q, block in enumerate(swap_chunks(blocks)):
            amplitude_ref[q, :, tile * LANES : (tile + 1) * LANES] = block
    place = place_ref[0]
    first = got_ref[place, CHUNK : CHUNK + 1]
    second = got_ref[place + 1, CHUNK : CHUNK + 1]
    stats_ref[...] = jnp.concatenate(
        [
            jnp.concatenate(
                [v[:, r * CHUNK : (r + 1) * CHUNK] for v in (first, second)], axis=1
            )
            for r in range(3)
        ],
        axis=0,
    )


def shards(coefficients, positions, shift_tables, absorb_weight, incident, detector):
    x, z = lax.axis_index("sph_0"), lax.axis_index("sph_1")
    y, core = lax.axis_index("ang_0"), lax.axis_index("ang_1")
    smem = pl.BlockSpec(memory_space=pltpu.SMEM)
    vmem = pl.BlockSpec(memory_space=pltpu.VMEM)

    mine, theirs = moved_sum(
        coefficients, positions, shift_tables, absorb_weight, core.astype(jnp.int32)
    )
    other = lax.ppermute(theirs, PAIR, [(0, 1), (1, 0)])
    (packed,) = call(pack_kernel, [struct((16, 64, LANES))], [mine, other, detector], "pack")
    packed, incident, z, y, core, polar = lax.optimization_barrier(
        (packed, incident, z, y, core, jnp.arange(POLAR))
    )
    (spread,) = call(
        plane_kernel,
        [struct((8, 72, LANES))],
        [lax.all_to_all(packed, PLANE, 0, 0, tiled=True)],
        "plane",
    )
    line = lax.all_to_all(spread, LINE, 0, 0, tiled=True)
    own = line[:, :64].sum(axis=0)
    partner = lax.ppermute(own, PAIR, [(0, 1), (1, 0)])

    degree, order, size, rise, fall, link, unit = index_tables()
    theta = (polar.astype(F32) + 0.5) * (math.pi / POLAR)
    cos_theta, sine_theta = jnp.cos(theta)[:, None], jnp.sin(theta)[:, None]
    whole = radial(cos_theta, sine_theta)
    solid_angle = 2.0 * math.pi * math.pi / (POLAR * AZIM)
    scaled = whole * (sine_theta * solid_angle)
    near_polar = ((jnp.arange(4) * 8 + z)[:, None] * 4 + jnp.arange(4)[None, :]).reshape(-1)
    near_theta = (near_polar.astype(F32) + 0.5) * (math.pi / POLAR)
    near = radial(jnp.cos(near_theta)[:, None], jnp.sin(near_theta)[:, None])
    near_azim = ((jnp.arange(4) * 2 + core)[:, None] * 8 + jnp.arange(8)[None, :]).reshape(-1)
    azimuth = near_azim.astype(F32) * (2.0 * math.pi / AZIM)
    angle = azimuth[:, None] * jnp.asarray(np.asarray(order, np.float32))[None, :]
    high, low = call(
        basis_kernel,
        [struct((2 * ROWS, 2 * ROWS), BF16)] * 2,
        [near, jnp.cos(angle), jnp.sin(angle)],
        "basis",
        flops=10_000_000,
    )
    turns = np.arange(AZIM)[:, None] * np.arange(2 * ORDER + 1)[None, :] % AZIM
    waves = np.zeros((AZIM, LANES), np.float32)
    waves[:, : 2 * ORDER + 1] = np.cos(2.0 * math.pi * turns / AZIM)
    waves[:, 64 : 64 + 2 * ORDER + 1] = np.sin(2.0 * math.pi * turns / AZIM)
    waves = np.tile(np.concatenate([waves[:CHUNK], waves[CHUNK:]], axis=1), (4, 1))
    gap = np.where((degree[:, None] > 0) & (degree[None, :] > 0), order[None, :] - order[:, None], 99)
    (form,) = call(
        power_kernel,
        [struct((2, LANES, 2 * LANES))],
        [whole, scaled, line, jnp.asarray(waves), jnp.asarray(gap.astype(np.int32))],
        "power",
        flops=1_000_000_000,
    )
    first = (4 * y + x) * CHUNK
    phase = np.stack([unit.real[:HALF], unit.imag[:HALF]]).astype(np.float32)
    phase = jnp.asarray(np.broadcast_to(phase[:, :, None], (2, HALF, LANES)))
    (messages,) = call(
        far_kernel,
        [struct((16, 40, LANES))],
        [
            core.astype(jnp.int32).reshape(1), own, partner, high, low, form, phase,
            lax.dynamic_slice_in_dim(incident, first, CHUNK, 1),
            lax.dynamic_slice_in_dim(incident, FIELDS + first, CHUNK, 1),
        ],
        "far",
        flops=400_000_000,
        in_specs=[smem] + [vmem] * 8,
    )
    got = lax.all_to_all(messages, PLANE, 0, 0, tiled=True)
    amplitude, stats = call(
        finish_kernel,
        [struct((4, 32, FIELDS)), struct((3, 64))],
        [(4 * y + 2 * core).astype(jnp.int32).reshape(1), got],
        "finish",
        in_specs=[smem, vmem],
    )
    return (amplitude.reshape(2, 2, 4, 8, FIELDS), stats)


def solution(mesh):
    torus = Mesh(mesh.devices.reshape(4, 8, 4, 2), SPH_ANG)
    in_specs = (P(SPH_ANG, None, None), P(SPH_ANG, None), P(), P(SPH_ANG, None), P(), P(SPH, None))
    out_specs = (P(None, None, SPH, ANG, None), P(None, ANG))
    return jax.shard_map(
        shards, mesh=torus, in_specs=in_specs, out_specs=out_specs, check_vma=False
    )
```

```python
import functools
import math

import jax
import jax.numpy as jnp
import numpy as np
from jax import lax
from jax.experimental import pallas as pl
from jax.experimental.pallas import tpu as pltpu
from jax.sharding import Mesh
from jax.sharding import PartitionSpec as P

ORDER = 10
AZIM = 64
POLAR = 128
COEFS = 240
HALF = 120
FIELDS = 512
ROWS = 256
CHUNK = 32
LANES = 128
SPH_ANG = ("sph_0", "sph_1", "ang_0", "ang_1")
SPH = ("sph_0", "sph_1")
ANG = ("ang_0", "ang_1")
PLANE = ("ang_0", "sph_0")
LINE = "sph_1"
PAIR = "ang_1"
F32 = jnp.float32
BF16 = jnp.bfloat16


def index_tables():
    degree, order = np.zeros(LANES), np.zeros(LANES)
    for n in range(1, ORDER + 1):
        for m in range(-n, n + 1):
            degree[n * n - 1 + n + m] = n
            order[n * n - 1 + n + m] = m
    size = np.abs(order)
    used = degree > 0
    rise, fall = np.zeros((ORDER + 1, LANES)), np.zeros((ORDER + 1, LANES))
    for t in range(1, ORDER + 1):
        on = used & (size < t) & (t <= degree)
        s = size[on]
        rise[t, on] = np.sqrt((4.0 * t * t - 1.0) / (t * t - s * s))
        if t > 1:
            fall[t, on] = np.sqrt(((t - 1.0) ** 2 - s * s) / (4.0 * (t - 1.0) ** 2 - 1.0))
    link = np.sqrt((2 * degree + 1) * (degree**2 - order**2) / np.maximum(2 * degree - 1, 1)) * used
    norm = used / np.sqrt(np.maximum(degree * (degree + 1.0), 1.0))
    unit = np.array([1.0, -1.0j, -1.0, 1.0j])[(degree.astype(int) + 1) % 4] * norm
    return degree, order, size, rise, fall, link, unit


def constants():
    degree, order, size, rise, fall, link, unit = index_tables()
    rows = [order, degree, size, link, unit.real, unit.imag, 0 * size, 0 * size]
    table = np.zeros((32, LANES), np.float32)
    table[:8] = np.stack(rows)
    table[8 : 8 + ORDER] = rise[1:]
    table[20 : 20 + ORDER] = fall[1:]
    return table


def radial(const_ref, theta):
    order, degree, size, link = (const_ref[r : r + 1] for r in range(4))
    cos_theta, sine_theta = jnp.cos(theta), jnp.sin(theta)
    current = jnp.full(theta.shape, 1.0 / math.sqrt(4.0 * math.pi), F32)
    for t in range(1, ORDER + 1):
        factor = -math.sqrt((2.0 * t + 1.0) / (2.0 * t))
        current = jnp.where(size >= t, factor * sine_theta * current, current)
    previous = jnp.zeros_like(current)
    for t in range(1, ORDER + 1):
        rise, fall = const_ref[7 + t : 8 + t], const_ref[19 + t : 20 + t]
        following = rise * (cos_theta * current - fall * previous)
        previous = jnp.where(rise > 0, current, previous)
        current = jnp.where(rise > 0, following, current)
    pi_term = order * current / sine_theta
    tau_term = (degree * cos_theta * current - link * previous) / sine_theta
    return tau_term + pi_term, tau_term - pi_term, sine_theta


def halves(value):
    high = value.astype(BF16)
    return high, (value - high.astype(F32)).astype(BF16)


def swap_chunks(blocks):
    group = lax.broadcasted_iota(jnp.int32, blocks[0].shape, 1) // CHUNK
    out = []
    for x in range(4):
        mixed = None
        for g in range(4):
            shift = (g - x) * CHUNK % LANES
            piece = pltpu.roll(blocks[g], shift, 1) if shift else blocks[g]
            mixed = piece if mixed is None else jnp.where(group == g, piece, mixed)
        out.append(mixed)
    return out


def call(body, outs, ins, flops=1, limit=16, **kw):
    size = sum(math.prod(a.shape) * a.dtype.itemsize for a in list(outs) + list(ins))
    return pl.pallas_call(
        body,
        out_shape=[jax.ShapeDtypeStruct(o.shape, o.dtype) for o in outs],
        compiler_params=pltpu.CompilerParams(vmem_limit_bytes=limit * 1024 * 1024),
        cost_estimate=pl.CostEstimate(flops=flops, bytes_accessed=size, transcendentals=0),
        **kw,
    )(*ins)


def struct(shape, dtype=F32):
    return jax.ShapeDtypeStruct(shape, dtype)


def move_kernel(
    unroll, core_ref, cell_ref, coef_hbm, table_hbm, weight_ref, mine_ref, theirs_ref,
    coef, table, total, absorbed, right, sems,
):
    spheres = coef.shape[0]
    groups = spheres // unroll

    def coef_copy(j):
        return pltpu.make_async_copy(coef_hbm.at[j], coef.at[j], sems.at[3, j])

    def table_copy(j, stage):
        axis = 2 - stage
        return pltpu.make_async_copy(
            table_hbm.at[axis, cell_ref[axis, j]], table.at[stage, j], sems.at[stage, j]
        )

    def fetches(group):
        own = range(group * unroll, (group + 1) * unroll)
        first = [copy for j in own for copy in (coef_copy(j), table_copy(j, 0))]
        return first, [table_copy(j, stage) for stage in (1, 2) for j in own]

    first, second = fetches(0)
    for copy in first + second:
        copy.start()
    total[...] = jnp.zeros_like(total)
    absorbed[...] = jnp.zeros_like(absorbed)
    weights = weight_ref[...].T
    for group in range(groups):
        if group + 1 < groups:
            ahead = fetches(group + 1)
            for copy in ahead[0] + ahead[1]:
                copy.start()
        for copy in first if group == 0 else first + second:
            copy.wait()
        for s in range(unroll):
            j = group * unroll + s
            real, imag = coef[j, :, :FIELDS].astype(F32), coef[j, :, FIELDS:].astype(F32)
            energy = (real * real + imag * imag) * weights[:, j : j + 1]
            absorbed[...] += jnp.sum(energy.reshape(COEFS // 8, 8, FIELDS), axis=0)
        for stage in range(3):
            if group == 0 and stage == 1:
                for copy in second:
                    copy.wait()
            for s in range(unroll):
                j = group * unroll + s
                matrix = table[stage, j]
                turned = jnp.concatenate([-matrix[COEFS:], matrix[:COEFS]], axis=0)
                if stage == 0:
                    real, imag = coef[j, :, :FIELDS], coef[j, :, FIELDS:]
                else:
                    real, imag = right[s, :COEFS], right[s, ROWS : ROWS + COEFS]
                product = jnp.dot(matrix, real, preferred_element_type=F32) + jnp.dot(
                    turned, imag, preferred_element_type=F32
                )
                if stage < 2:
                    product = product.astype(BF16)
                    right[s, :COEFS] = product[:COEFS]
                    right[s, ROWS : ROWS + COEFS] = product[COEFS:]
                else:
                    total[0, :COEFS] += product[:COEFS]
                    total[1, :COEFS] += product[COEFS:]
        if group + 1 < groups:
            first, second = ahead
    total[0, COEFS : COEFS + 1] = jnp.sum(absorbed[...], axis=0, keepdims=True)
    core = core_ref[0]
    for part, out_ref in ((core, mine_ref), (1 - core, theirs_ref)):
        for tile in range(4):
            lanes = slice(tile * LANES, (tile + 1) * LANES)
            blocks = [total[part, g * 64 : (g + 1) * 64, lanes] for g in range(4)]
            for x, block in enumerate(swap_chunks(blocks)):
                out_ref[4 * tile + x] = block


def moved_sum(coefficients, positions, shift_tables, absorb_weight, core, unroll=2):
    spheres = coefficients.shape[0]
    smem = pl.BlockSpec(memory_space=pltpu.SMEM)
    hbm = pl.BlockSpec(memory_space=pltpu.HBM)
    vmem = pl.BlockSpec(memory_space=pltpu.VMEM)
    return pl.pallas_call(
        functools.partial(move_kernel, unroll),
        in_specs=[smem, smem, hbm, hbm, vmem],
        out_specs=[vmem, vmem],
        scratch_shapes=[
            pltpu.VMEM((spheres, COEFS, 2 * FIELDS), BF16),
            pltpu.VMEM((3, spheres, 2 * COEFS, COEFS), BF16),
            pltpu.VMEM((2, ROWS, FIELDS), F32),
            pltpu.VMEM((8, FIELDS), F32),
            pltpu.VMEM((unroll, 2 * ROWS, FIELDS), BF16),
            pltpu.SemaphoreType.DMA((4, spheres)),
        ],
        out_shape=[struct((16, 64, LANES))] * 2,
        compiler_params=pltpu.CompilerParams(vmem_limit_bytes=52 * 1024 * 1024),
        cost_estimate=pl.CostEstimate(
            flops=6_000_000_000, bytes_accessed=10_000_000, transcendentals=0
        ),
        name="move",
    )(core, positions.T, coefficients, shift_tables, absorb_weight)


def plane_kernel(got_ref, out_ref):
    total = got_ref[0]
    for k in range(1, 16):
        total = total + got_ref[k]
    group = lax.broadcasted_iota(jnp.int32, (8, LANES), 1) // CHUNK
    detectors = got_ref[3, 56:]
    for x in range(3):
        detectors = jnp.where(
            group == x, pltpu.roll(got_ref[x, 56:], (x + 1) * CHUNK, 1), detectors
        )
    for k in range(8):
        out_ref[k, :64] = total
        out_ref[k, 64:] = detectors


def tables_kernel(
    place_ref, const_ref, high_ref, low_ref, whole_ref, scaled_ref, gap_ref, waves_ref, phase_ref
):
    z, core = place_ref[0], place_ref[1]
    row = lambda shape: lax.broadcasted_iota(jnp.int32, shape, 0)
    step = math.pi / POLAR

    near = row((16, LANES))
    near = ((near // 4) * 8 + z) * 4 + near % 4
    plus, minus, _ = radial(const_ref, (near.astype(F32) + 0.5) * step)
    azim = row((32, LANES))
    azim = ((azim // 8) * 2 + core) * 8 + azim % 8
    turn = (azim * const_ref[0:1].astype(jnp.int32)) & (AZIM - 1)
    angle = turn.astype(F32) * (2.0 * math.pi / AZIM)
    for sign, table in enumerate((plus, minus)):
        for trig, wave in enumerate((jnp.cos(angle), jnp.sin(angle))):
            block = table[None, :, None, :] * wave.reshape(4, 1, 8, LANES)
            high, low = halves(block.reshape(2 * ROWS, LANES))
            lanes = slice((2 * sign + trig) * LANES, (2 * sign + trig + 1) * LANES)
            high_ref[:, lanes] = high
            low_ref[:, lanes] = low

    plus, minus, sine_theta = radial(
        const_ref, (row((POLAR, LANES)).astype(F32) + 0.5) * step
    )
    weight = sine_theta * (2.0 * math.pi * math.pi / (POLAR * AZIM))
    for sign, table in enumerate((plus, minus)):
        whole_ref[sign] = table
        scaled_ref[sign] = table * weight

    across = lambda r: jnp.broadcast_to(const_ref[r : r + 1], (LANES, LANES))
    used = across(1) > 0
    order = across(0)
    gap = jnp.where(used, order, 200.0) - jnp.where(used, order, 100.0).T
    gap_ref[...] = gap
    phase_ref[0] = across(4).T
    phase_ref[1] = across(5).T

    shape = (LANES, LANES)
    lane = lax.broadcasted_iota(jnp.int32, shape, 1)
    for half in range(2):
        azim = row(shape) % CHUNK + half * CHUNK
        turn = (azim * (lane % 64) - jnp.where(lane < 64, 0, AZIM // 4)) & (AZIM - 1)
        wave = jnp.cos(turn.astype(F32) * (2.0 * math.pi / AZIM))
        waves_ref[:, half * LANES : (half + 1) * LANES] = wave


def power_kernel(radial_ref, scaled_ref, line_ref, waves_ref, gap_ref, out_ref):
    gap = gap_ref[...]
    far = jnp.abs(gap)
    far = jnp.concatenate([far, far], axis=1)
    detectors = line_ref[:, 64:].reshape(64, LANES)
    group = lax.broadcasted_iota(jnp.int32, detectors.shape, 1) // CHUNK
    detectors = jnp.concatenate([jnp.where(group == x, detectors, 0.0) for x in range(4)], axis=0)
    spectrum = jnp.dot(
        detectors, waves_ref[...], preferred_element_type=F32, precision=lax.Precision.HIGHEST
    )
    spectrum = spectrum[:, :LANES] + pltpu.roll(spectrum[:, LANES:], 2 * LANES - 4, 0)
    spectrum = jnp.concatenate([spectrum[8 * k : 8 * k + 4] for k in range(32)], axis=0)
    for sign in range(2):
        table = scaled_ref[sign]
        left_high, left_low = halves(radial_ref[sign].T)
        left = jnp.concatenate([left_high, left_high], axis=1)
        total = jnp.zeros((LANES, 2 * LANES), F32)
        for d in range(2 * ORDER + 1):
            right = jnp.concatenate(
                [table * spectrum[:, d : d + 1], table * spectrum[:, 64 + d : 65 + d]], axis=1
            )
            high, low = halves(right)
            product = jnp.dot(
                left, jnp.concatenate([high, low], axis=0), preferred_element_type=F32
            ) + jnp.dot(left_low, high, preferred_element_type=F32)
            total = jnp.where(far == d, product, total)
        out_ref[sign, :, :LANES] = total[:, :LANES]
        out_ref[sign, :, LANES:] = jnp.where(gap < 0, -total[:, LANES:], total[:, LANES:])


def spread_rows(packed):
    parts = [packed] + [pltpu.roll(packed, LANES - g * CHUNK, 1) for g in (1, 2, 3)]
    return jnp.concatenate(parts, axis=0)


def columns(group, pieces):
    out = pieces[0]
    for g in (1, 2, 3):
        out = jnp.where(group == g, pltpu.roll(pieces[g], g * CHUNK, 1), out)
    return out


def far_kernel(
    core_ref, own_ref, other_ref, high_ref, low_ref, form_ref, phase_ref,
    incident_ref, incident_imag_ref, out_ref,
):
    core = core_ref[0]
    own, other = own_ref[...], other_ref[...]
    real = spread_rows(jnp.where(core == 0, own, other))
    imag = spread_rows(jnp.where(core == 0, other, own))
    group = lax.broadcasted_iota(jnp.int32, (HALF, LANES), 1) // CHUNK
    spare = jnp.zeros((8, LANES), F32)
    phase_real, phase_imag = phase_ref[0, :HALF], phase_ref[1, :HALF]
    real_1, real_2 = real[:HALF], real[HALF:COEFS]
    imag_1, imag_2 = imag[:HALF], imag[HALF:COEFS]
    rows = []
    collected = jnp.zeros((1, LANES), F32)
    for sign in range(2):
        if sign == 0:
            both = (real_2 - imag_1, imag_2 + real_1)
        else:
            both = (real_2 + imag_1, imag_2 - real_1)
        re = phase_real * both[0] - phase_imag * both[1]
        im = phase_real * both[1] + phase_imag * both[0]
        if sign == 0:
            top = columns(group, (re, im, -im, re))
            low = columns(group, (-im, re, -re, -im))
        else:
            top = columns(group, (re, im, im, -re))
            low = columns(group, (-im, re, re, im))
        rows += [0.5 * top, spare, 0.5 * low, spare]
        pair = jnp.concatenate([jnp.where(group == 0, re, 0.0), spare], axis=0)
        pair_imag = jnp.concatenate([jnp.where(group == 0, im, 0.0), spare], axis=0)
        dot = functools.partial(
            jnp.dot, preferred_element_type=F32, precision=lax.Precision.HIGHEST
        )
        even, odd = form_ref[sign, :, :LANES], form_ref[sign, :, LANES:]
        collected += 0.5 * jnp.sum(
            pair * dot(even, pair)
            + pair_imag * (dot(even, pair_imag) + 2.0 * dot(odd, pair)),
            axis=0,
            keepdims=True,
        )
    high, low = halves(jnp.concatenate(rows, axis=0))
    wide = jnp.dot(
        high_ref[...], jnp.concatenate([high, low], axis=1), preferred_element_type=F32
    )
    result = (
        wide[:, :LANES]
        + wide[:, LANES:]
        + jnp.dot(low_ref[...], high, preferred_element_type=F32)
    )
    extinction = jnp.sum(
        incident_ref[...] * real[:COEFS, :CHUNK] + incident_imag_ref[...] * imag[:COEFS, :CHUNK],
        axis=0,
        keepdims=True,
    )
    stats = jnp.concatenate(
        [
            extinction,
            real[COEFS : COEFS + 1, :CHUNK],
            collected[:, :CHUNK],
            jnp.zeros((1, CHUNK), F32),
        ],
        axis=1,
    )
    stats = jnp.broadcast_to(stats, (8, LANES))
    for k in range(16):
        out_ref[k, :CHUNK] = result[k * CHUNK : (k + 1) * CHUNK]
        out_ref[k, CHUNK:] = stats


def finish_kernel(place_ref, got_ref, amplitude_ref, stats_ref):
    for tile in range(4):
        blocks = [got_ref[4 * tile + x, :CHUNK] for x in range(4)]
        for q, block in enumerate(swap_chunks(blocks)):
            amplitude_ref[q, :, tile * LANES : (tile + 1) * LANES] = block
    place = place_ref[0]
    first = got_ref[place, CHUNK : CHUNK + 1]
    second = got_ref[place + 1, CHUNK : CHUNK + 1]
    stats_ref[...] = jnp.concatenate(
        [
            jnp.concatenate(
                [v[:, r * CHUNK : (r + 1) * CHUNK] for v in (first, second)], axis=1
            )
            for r in range(3)
        ],
        axis=0,
    )


def shards(coefficients, positions, shift_tables, absorb_weight, incident, detector):
    x, z = lax.axis_index("sph_0"), lax.axis_index("sph_1")
    y, core = lax.axis_index("ang_0"), lax.axis_index("ang_1")
    smem = pl.BlockSpec(memory_space=pltpu.SMEM)
    vmem = pl.BlockSpec(memory_space=pltpu.VMEM)

    mine, theirs = moved_sum(
        coefficients, positions, shift_tables, absorb_weight, core.reshape(1)
    )
    other = lax.ppermute(theirs, PAIR, [(0, 1), (1, 0)])
    share = jnp.concatenate([detector[:, :CHUNK], detector[:, CHUNK:]], axis=0)
    packed = mine + other + jnp.pad(share, ((56, 0), (96, 0)))[None]
    packed, incident, x, z, y, core = lax.optimization_barrier(
        (packed, incident, x, z, y, core)
    )
    high, low, whole, scaled, gap, waves, phase = call(
        tables_kernel,
        [
            struct((2 * ROWS, 2 * ROWS), BF16), struct((2 * ROWS, 2 * ROWS), BF16),
            struct((2, POLAR, LANES)), struct((2, POLAR, LANES)), struct((LANES, LANES)),
            struct((LANES, 2 * LANES)), struct((2, LANES, LANES)),
        ],
        [jnp.stack([z, core]), jnp.asarray(constants())],
        flops=100_000_000,
        in_specs=[smem, vmem],
    )
    first = (4 * y + x) * CHUNK
    tables = (
        whole, scaled, waves, gap, high, low, phase,
        lax.dynamic_slice_in_dim(incident, first, CHUNK, 1),
        lax.dynamic_slice_in_dim(incident, FIELDS + first, CHUNK, 1),
        core.astype(jnp.int32).reshape(1), (4 * y + 2 * core).astype(jnp.int32).reshape(1),
    )
    got = lax.all_to_all(packed, PLANE, 0, 0, tiled=True)
    got, tables = lax.optimization_barrier((got, tables))
    whole, scaled, waves, gap, high, low, phase, inc_real, inc_imag, core, place = tables
    (spread,) = call(plane_kernel, [struct((8, 72, LANES))], [got])
    line = lax.all_to_all(spread, LINE, 0, 0, tiled=True)
    own = line[:, :64].sum(axis=0)
    partner = lax.ppermute(own, PAIR, [(0, 1), (1, 0)])
    (form,) = call(
        power_kernel,
        [struct((2, LANES, 2 * LANES))],
        [whole, scaled, line, waves, gap],
        flops=1_000_000_000,
    )
    (messages,) = call(
        far_kernel,
        [struct((16, 40, LANES))],
        [core, own, partner, high, low, form, phase, inc_real, inc_imag],
        flops=400_000_000,
        in_specs=[smem] + [vmem] * 8,
    )
    got = lax.all_to_all(messages, PLANE, 0, 0, tiled=True)
    amplitude, stats = call(
        finish_kernel,
        [struct((4, 32, FIELDS)), struct((3, 64))],
        [place, got],
        in_specs=[smem, vmem],
    )
    return (amplitude.reshape(2, 2, 4, 8, FIELDS), stats)


def solution(mesh):
    torus = Mesh(mesh.devices.reshape(4, 8, 4, 2), SPH_ANG)
    in_specs = (P(SPH_ANG, None, None), P(SPH_ANG, None), P(), P(SPH_ANG, None), P(), P(SPH, None))
    out_specs = (P(None, None, SPH, ANG, None), P(None, ANG))
    return jax.shard_map(
        shards, mesh=torus, in_specs=in_specs, out_specs=out_specs, check_vma=False
    )
```

```python
import functools
import math

import jax
import jax.numpy as jnp
import numpy as np
from jax import lax
from jax.experimental import pallas as pl
from jax.experimental.pallas import tpu as pltpu
from jax.sharding import Mesh
from jax.sharding import PartitionSpec as P

ORDER = 10
AZIM = 64
POLAR = 128
COEFS = 240
HALF = 120
FIELDS = 512
ROWS = 256
CHUNK = 32
LANES = 128
SPH_ANG = ("sph_0", "sph_1", "ang_0", "ang_1")
SPH = ("sph_0", "sph_1")
ANG = ("ang_0", "ang_1")
PLANE = ("ang_0", "sph_0")
LINE = "sph_1"
PAIR = "ang_1"
F32 = jnp.float32
BF16 = jnp.bfloat16


def index_tables():
    degree, order = np.zeros(LANES), np.zeros(LANES)
    for n in range(1, ORDER + 1):
        for m in range(-n, n + 1):
            degree[n * n - 1 + n + m] = n
            order[n * n - 1 + n + m] = m
    size = np.abs(order)
    used = degree > 0
    rise, fall = np.zeros((ORDER + 1, LANES)), np.zeros((ORDER + 1, LANES))
    for t in range(1, ORDER + 1):
        on = used & (size < t) & (t <= degree)
        s = size[on]
        rise[t, on] = np.sqrt((4.0 * t * t - 1.0) / (t * t - s * s))
        if t > 1:
            fall[t, on] = np.sqrt(((t - 1.0) ** 2 - s * s) / (4.0 * (t - 1.0) ** 2 - 1.0))
    link = np.sqrt((2 * degree + 1) * (degree**2 - order**2) / np.maximum(2 * degree - 1, 1)) * used
    norm = used / np.sqrt(np.maximum(degree * (degree + 1.0), 1.0))
    unit = np.array([1.0, -1.0j, -1.0, 1.0j])[(degree.astype(int) + 1) % 4] * norm
    return degree, order, size, rise, fall, link, unit


def constants():
    degree, order, size, rise, fall, link, unit = index_tables()
    rows = [order, degree, size, link, unit.real, unit.imag, 0 * size, 0 * size]
    table = np.zeros((32, LANES), np.float32)
    table[:8] = np.stack(rows)
    table[8 : 8 + ORDER] = rise[1:]
    table[20 : 20 + ORDER] = fall[1:]
    return table


def radial(const_ref, theta):
    order, degree, size, link = (const_ref[r : r + 1] for r in range(4))
    cos_theta, sine_theta = jnp.cos(theta), jnp.sin(theta)
    current = jnp.full(theta.shape, 1.0 / math.sqrt(4.0 * math.pi), F32)
    for t in range(1, ORDER + 1):
        factor = -math.sqrt((2.0 * t + 1.0) / (2.0 * t))
        current = jnp.where(size >= t, factor * sine_theta * current, current)
    previous = jnp.zeros_like(current)
    for t in range(1, ORDER + 1):
        rise, fall = const_ref[7 + t : 8 + t], const_ref[19 + t : 20 + t]
        following = rise * (cos_theta * current - fall * previous)
        previous = jnp.where(rise > 0, current, previous)
        current = jnp.where(rise > 0, following, current)
    pi_term = order * current / sine_theta
    tau_term = (degree * cos_theta * current - link * previous) / sine_theta
    return tau_term + pi_term, tau_term - pi_term, sine_theta


def halves(value):
    high = value.astype(BF16)
    return high, (value - high.astype(F32)).astype(BF16)


def swap_chunks(blocks):
    group = lax.broadcasted_iota(jnp.int32, blocks[0].shape, 1) // CHUNK
    out = []
    for x in range(4):
        mixed = None
        for g in range(4):
            shift = (g - x) * CHUNK % LANES
            piece = pltpu.roll(blocks[g], shift, 1) if shift else blocks[g]
            mixed = piece if mixed is None else jnp.where(group == g, piece, mixed)
        out.append(mixed)
    return out


def call(body, outs, ins, flops=1, limit=16, **kw):
    size = sum(math.prod(a.shape) * a.dtype.itemsize for a in list(outs) + list(ins))
    return pl.pallas_call(
        body,
        out_shape=[jax.ShapeDtypeStruct(o.shape, o.dtype) for o in outs],
        compiler_params=pltpu.CompilerParams(vmem_limit_bytes=limit * 1024 * 1024),
        cost_estimate=pl.CostEstimate(flops=flops, bytes_accessed=size, transcendentals=0),
        **kw,
    )(*ins)


def struct(shape, dtype=F32):
    return jax.ShapeDtypeStruct(shape, dtype)


def pack(total, part, out_ref):
    for tile in range(4):
        lanes = slice(tile * LANES, (tile + 1) * LANES)
        blocks = [total[part, g * 64 : (g + 1) * 64, lanes] for g in range(4)]
        for x, block in enumerate(swap_chunks(blocks)):
            out_ref[4 * tile + x] = block


def pack_kernel(core_ref, total_ref, detector_ref, out_ref):
    pack(total_ref, core_ref[0], out_ref)
    detector = detector_ref[...]
    detector = jnp.concatenate([detector[:, :CHUNK], detector[:, CHUNK:]], axis=0)
    for k in range(16):
        out_ref[k, 56:, 96:] = detector


def move_kernel(
    unroll, core_ref, cell_ref, coef_hbm, table_hbm, weight_ref, total, theirs_ref,
    coef, table, absorbed, right, sems,
):
    spheres = coef.shape[0]
    groups = spheres // unroll

    def coef_copy(j):
        return pltpu.make_async_copy(coef_hbm.at[j], coef.at[j], sems.at[3, j])

    def table_copy(j, stage):
        axis = 2 - stage
        return pltpu.make_async_copy(
            table_hbm.at[axis, cell_ref[axis, j]], table.at[stage, j], sems.at[stage, j]
        )

    def fetches(group):
        own = range(group * unroll, (group + 1) * unroll)
        first = [copy for j in own for copy in (coef_copy(j), table_copy(j, 0))]
        return first, [table_copy(j, stage) for stage in (1, 2) for j in own]

    first, second = fetches(0)
    for copy in first + second:
        copy.start()
    total[...] = jnp.zeros_like(total)
    absorbed[...] = jnp.zeros_like(absorbed)
    weights = weight_ref[...].T
    for group in range(groups):
        if group + 1 < groups:
            ahead = fetches(group + 1)
            for copy in ahead[0] + ahead[1]:
                copy.start()
        for copy in first if group == 0 else first + second:
            copy.wait()
        for s in range(unroll):
            j = group * unroll + s
            real, imag = coef[j, :, :FIELDS].astype(F32), coef[j, :, FIELDS:].astype(F32)
            energy = (real * real + imag * imag) * weights[:, j : j + 1]
            absorbed[...] += jnp.sum(energy.reshape(COEFS // 8, 8, FIELDS), axis=0)
        for stage in range(3):
            if group == 0 and stage == 1:
                for copy in second:
                    copy.wait()
            for s in range(unroll):
                j = group * unroll + s
                matrix = table[stage, j]
                turned = jnp.concatenate([-matrix[COEFS:], matrix[:COEFS]], axis=0)
                if stage == 0:
                    real, imag = coef[j, :, :FIELDS], coef[j, :, FIELDS:]
                else:
                    real, imag = right[s, :COEFS], right[s, ROWS : ROWS + COEFS]
                product = jnp.dot(matrix, real, preferred_element_type=F32) + jnp.dot(
                    turned, imag, preferred_element_type=F32
                )
                if stage < 2:
                    product = product.astype(BF16)
                    right[s, :COEFS] = product[:COEFS]
                    right[s, ROWS : ROWS + COEFS] = product[COEFS:]
                else:
                    total[0, :COEFS] += product[:COEFS]
                    total[1, :COEFS] += product[COEFS:]
        if group + 1 < groups:
            first, second = ahead
    total[0, COEFS : COEFS + 1] = jnp.sum(absorbed[...], axis=0, keepdims=True)
    pack(total, 1 - core_ref[0], theirs_ref)


def moved_sum(coefficients, positions, shift_tables, absorb_weight, core, unroll=2):
    spheres = coefficients.shape[0]
    smem = pl.BlockSpec(memory_space=pltpu.SMEM)
    hbm = pl.BlockSpec(memory_space=pltpu.HBM)
    vmem = pl.BlockSpec(memory_space=pltpu.VMEM)
    return pl.pallas_call(
        functools.partial(move_kernel, unroll),
        in_specs=[smem, smem, hbm, hbm, vmem],
        out_specs=[vmem, vmem],
        scratch_shapes=[
            pltpu.VMEM((spheres, COEFS, 2 * FIELDS), BF16),
            pltpu.VMEM((3, spheres, 2 * COEFS, COEFS), BF16),
            pltpu.VMEM((8, FIELDS), F32),
            pltpu.VMEM((unroll, 2 * ROWS, FIELDS), BF16),
            pltpu.SemaphoreType.DMA((4, spheres)),
        ],
        out_shape=[struct((2, ROWS, FIELDS)), struct((16, 64, LANES))],
        compiler_params=pltpu.CompilerParams(vmem_limit_bytes=52 * 1024 * 1024),
        cost_estimate=pl.CostEstimate(
            flops=6_000_000_000, bytes_accessed=10_000_000, transcendentals=0
        ),
        name="move",
    )(core, positions.T, coefficients, shift_tables, absorb_weight)


def plane_kernel(got_ref, out_ref):
    total = got_ref[0]
    for k in range(1, 16):
        total = total + got_ref[k]
    group = lax.broadcasted_iota(jnp.int32, (8, LANES), 1) // CHUNK
    detectors = got_ref[3, 56:]
    for x in range(3):
        detectors = jnp.where(
            group == x, pltpu.roll(got_ref[x, 56:], (x + 1) * CHUNK, 1), detectors
        )
    for k in range(8):
        out_ref[k, :64] = total
        out_ref[k, 64:] = detectors


def tables_kernel(
    place_ref, const_ref, high_ref, low_ref, whole_ref, scaled_ref, gap_ref, waves_ref, phase_ref
):
    z, core = place_ref[0], place_ref[1]
    row = lambda shape: lax.broadcasted_iota(jnp.int32, shape, 0)
    step = math.pi / POLAR

    near = row((16, LANES))
    near = ((near // 4) * 8 + z) * 4 + near % 4
    plus, minus, _ = radial(const_ref, (near.astype(F32) + 0.5) * step)
    azim = row((32, LANES))
    azim = ((azim // 8) * 2 + core) * 8 + azim % 8
    turn = (azim * const_ref[0:1].astype(jnp.int32)) & (AZIM - 1)
    angle = turn.astype(F32) * (2.0 * math.pi / AZIM)
    for sign, table in enumerate((plus, minus)):
        for trig, wave in enumerate((jnp.cos(angle), jnp.sin(angle))):
            block = table[None, :, None, :] * wave.reshape(4, 1, 8, LANES)
            high, low = halves(block.reshape(2 * ROWS, LANES))
            lanes = slice((2 * sign + trig) * LANES, (2 * sign + trig + 1) * LANES)
            high_ref[:, lanes] = high
            low_ref[:, lanes] = low

    plus, minus, sine_theta = radial(
        const_ref, (row((POLAR, LANES)).astype(F32) + 0.5) * step
    )
    weight = sine_theta * (2.0 * math.pi * math.pi / (POLAR * AZIM))
    for sign, table in enumerate((plus, minus)):
        whole_ref[sign] = table
        scaled_ref[sign] = table * weight

    across = lambda r: jnp.broadcast_to(const_ref[r : r + 1], (LANES, LANES))
    used = across(1) > 0
    order = across(0)
    gap = jnp.where(used, order, 200.0) - jnp.where(used, order, 100.0).T
    gap_ref[...] = gap
    phase_ref[0] = across(4).T
    phase_ref[1] = across(5).T

    shape = (LANES, LANES)
    lane = lax.broadcasted_iota(jnp.int32, shape, 1)
    for half in range(2):
        azim = row(shape) % CHUNK + half * CHUNK
        turn = (azim * (lane % 64) - jnp.where(lane < 64, 0, AZIM // 4)) & (AZIM - 1)
        wave = jnp.cos(turn.astype(F32) * (2.0 * math.pi / AZIM))
        waves_ref[:, half * LANES : (half + 1) * LANES] = wave


def power_kernel(radial_ref, scaled_ref, line_ref, waves_ref, gap_ref, out_ref):
    gap = gap_ref[...]
    detectors = line_ref[:, 64:].reshape(64, LANES)
    group = lax.broadcasted_iota(jnp.int32, detectors.shape, 1) // CHUNK
    detectors = jnp.concatenate([jnp.where(group == x, detectors, 0.0) for x in range(4)], axis=0)
    spectrum = jnp.dot(
        detectors, waves_ref[...], preferred_element_type=F32, precision=lax.Precision.HIGHEST
    )
    spectrum = spectrum[:, :LANES] + pltpu.roll(spectrum[:, LANES:], 2 * LANES - 4, 0)
    spectrum = jnp.concatenate([spectrum[8 * k : 8 * k + 4] for k in range(32)], axis=0)
    spectrum = spectrum.T
    far = jnp.abs(gap[:HALF])
    far = jnp.concatenate([far, far], axis=0)
    for sign in range(2):
        table = scaled_ref[sign].T[:HALF]
        high, low = halves(radial_ref[sign])
        fixed = jnp.concatenate([high, low], axis=1)
        fixed = jnp.concatenate([fixed, fixed], axis=0)
        total = jnp.zeros((COEFS, LANES), F32)
        for start in range(0, 2 * ORDER + 1, 7):
            rows = []
            for d in range(start, start + 7):
                rows += [table * spectrum[d : d + 1], table * spectrum[64 + d : 65 + d]]
            high, low = halves(jnp.concatenate(rows, axis=0))
            product = jnp.dot(
                jnp.concatenate([high, low], axis=1), fixed, preferred_element_type=F32
            )
            product = product[:, :LANES] + product[:, LANES:]
            for k in range(7):
                part = product[k * COEFS : (k + 1) * COEFS]
                total = jnp.where(far == start + k, part, total)
        out_ref[sign, 0, :HALF] = total[:HALF]
        out_ref[sign, 1, :HALF] = jnp.where(gap[:HALF] < 0, -total[HALF:], total[HALF:])
        out_ref[sign, :, HALF:] = jnp.zeros((2, 8, LANES), F32)


def spread_rows(packed):
    parts = [packed] + [pltpu.roll(packed, LANES - g * CHUNK, 1) for g in (1, 2, 3)]
    return jnp.concatenate(parts, axis=0)


def columns(group, pieces):
    out = pieces[0]
    for g in (1, 2, 3):
        out = jnp.where(group == g, pltpu.roll(pieces[g], g * CHUNK, 1), out)
    return out


def far_kernel(
    core_ref, own_ref, other_ref, high_ref, low_ref, form_ref, phase_ref,
    incident_ref, incident_imag_ref, out_ref,
):
    core = core_ref[0]
    own, other = own_ref[...], other_ref[...]
    real = spread_rows(jnp.where(core == 0, own, other))
    imag = spread_rows(jnp.where(core == 0, other, own))
    group = lax.broadcasted_iota(jnp.int32, (HALF, LANES), 1) // CHUNK
    spare = jnp.zeros((8, LANES), F32)
    phase_real, phase_imag = phase_ref[0, :HALF], phase_ref[1, :HALF]
    real_1, real_2 = real[:HALF], real[HALF:COEFS]
    imag_1, imag_2 = imag[:HALF], imag[HALF:COEFS]
    rows = []
    collected = jnp.zeros((1, LANES), F32)
    for sign in range(2):
        if sign == 0:
            both = (real_2 - imag_1, imag_2 + real_1)
        else:
            both = (real_2 + imag_1, imag_2 - real_1)
        re = phase_real * both[0] - phase_imag * both[1]
        im = phase_real * both[1] + phase_imag * both[0]
        if sign == 0:
            top = columns(group, (re, im, -im, re))
            low = columns(group, (-im, re, -re, -im))
        else:
            top = columns(group, (re, im, im, -re))
            low = columns(group, (-im, re, re, im))
        rows += [0.5 * top, spare, 0.5 * low, spare]
        pair = jnp.concatenate([jnp.where(group == 0, re, 0.0), spare], axis=0)
        pair_imag = jnp.concatenate([jnp.where(group == 0, im, 0.0), spare], axis=0)
        dot = functools.partial(
            jnp.dot, preferred_element_type=F32, precision=lax.Precision.HIGHEST
        )
        even, odd = form_ref[sign, 0], form_ref[sign, 1]
        collected += 0.5 * jnp.sum(
            pair * dot(even, pair)
            + pair_imag * (dot(even, pair_imag) + 2.0 * dot(odd, pair)),
            axis=0,
            keepdims=True,
        )
    high, low = halves(jnp.concatenate(rows, axis=0))
    wide = jnp.dot(
        high_ref[...], jnp.concatenate([high, low], axis=1), preferred_element_type=F32
    )
    result = (
        wide[:, :LANES]
        + wide[:, LANES:]
        + jnp.dot(low_ref[...], high, preferred_element_type=F32)
    )
    extinction = jnp.sum(
        incident_ref[...] * real[:COEFS, :CHUNK] + incident_imag_ref[...] * imag[:COEFS, :CHUNK],
        axis=0,
        keepdims=True,
    )
    stats = jnp.concatenate(
        [
            extinction,
            real[COEFS : COEFS + 1, :CHUNK],
            collected[:, :CHUNK],
            jnp.zeros((1, CHUNK), F32),
        ],
        axis=1,
    )
    stats = jnp.broadcast_to(stats, (8, LANES))
    for k in range(16):
        out_ref[k, :CHUNK] = result[k * CHUNK : (k + 1) * CHUNK]
        out_ref[k, CHUNK:] = stats


def finish_kernel(place_ref, got_ref, amplitude_ref, stats_ref):
    for tile in range(4):
        blocks = [got_ref[4 * tile + x, :CHUNK] for x in range(4)]
        for q, block in enumerate(swap_chunks(blocks)):
            amplitude_ref[q, :, tile * LANES : (tile + 1) * LANES] = block
    place = place_ref[0]
    first = got_ref[place, CHUNK : CHUNK + 1]
    second = got_ref[place + 1, CHUNK : CHUNK + 1]
    stats_ref[...] = jnp.concatenate(
        [
            jnp.concatenate(
                [v[:, r * CHUNK : (r + 1) * CHUNK] for v in (first, second)], axis=1
            )
            for r in range(3)
        ],
        axis=0,
    )


def shards(coefficients, positions, shift_tables, absorb_weight, incident, detector):
    x, z = lax.axis_index("sph_0"), lax.axis_index("sph_1")
    y, core = lax.axis_index("ang_0"), lax.axis_index("ang_1")
    smem = pl.BlockSpec(memory_space=pltpu.SMEM)
    vmem = pl.BlockSpec(memory_space=pltpu.VMEM)

    total, theirs = moved_sum(
        coefficients, positions, shift_tables, absorb_weight, core.reshape(1)
    )
    other = lax.ppermute(theirs, PAIR, [(0, 1), (1, 0)])
    (mine,) = call(
        pack_kernel,
        [struct((16, 64, LANES))],
        [core.reshape(1), total, detector],
        flops=10_000_000,
        in_specs=[smem, vmem, vmem],
    )
    packed = mine + other
    packed, incident, x, z, y, core = lax.optimization_barrier(
        (packed, incident, x, z, y, core)
    )
    high, low, whole, scaled, gap, waves, phase = call(
        tables_kernel,
        [
            struct((2 * ROWS, 2 * ROWS), BF16), struct((2 * ROWS, 2 * ROWS), BF16),
            struct((2, POLAR, LANES)), struct((2, POLAR, LANES)), struct((LANES, LANES)),
            struct((LANES, 2 * LANES)), struct((2, LANES, LANES)),
        ],
        [jnp.stack([z, core]), jnp.asarray(constants())],
        flops=100_000_000,
        in_specs=[smem, vmem],
    )
    first = (4 * y + x) * CHUNK
    tables = (
        whole, scaled, waves, gap, high, low, phase,
        lax.dynamic_slice_in_dim(incident, first, CHUNK, 1),
        lax.dynamic_slice_in_dim(incident, FIELDS + first, CHUNK, 1),
        core.astype(jnp.int32).reshape(1), (4 * y + 2 * core).astype(jnp.int32).reshape(1),
    )
    got = lax.all_to_all(packed, PLANE, 0, 0, tiled=True)
    got, tables = lax.optimization_barrier((got, tables))
    whole, scaled, waves, gap, high, low, phase, inc_real, inc_imag, core, place = tables
    (spread,) = call(plane_kernel, [struct((8, 72, LANES))], [got])
    line = lax.all_to_all(spread, LINE, 0, 0, tiled=True)
    own = line[:, :64].sum(axis=0)
    partner = lax.ppermute(own, PAIR, [(0, 1), (1, 0)])
    (form,) = call(
        power_kernel,
        [struct((2, 2, LANES, LANES))],
        [whole, scaled, line, waves, gap],
        flops=1_000_000_000,
    )
    (messages,) = call(
        far_kernel,
        [struct((16, 40, LANES))],
        [core, own, partner, high, low, form, phase, inc_real, inc_imag],
        flops=400_000_000,
        in_specs=[smem] + [vmem] * 8,
    )
    got = lax.all_to_all(messages, PLANE, 0, 0, tiled=True)
    amplitude, stats = call(
        finish_kernel,
        [struct((4, 32, FIELDS)), struct((3, 64))],
        [place, got],
        in_specs=[smem, vmem],
    )
    return (amplitude.reshape(2, 2, 4, 8, FIELDS), stats)


def solution(mesh):
    torus = Mesh(mesh.devices.reshape(4, 8, 4, 2), SPH_ANG)
    in_specs = (P(SPH_ANG, None, None), P(SPH_ANG, None), P(), P(SPH_ANG, None), P(), P(SPH, None))
    out_specs = (P(None, None, SPH, ANG, None), P(None, ANG))
    return jax.shard_map(
        shards, mesh=torus, in_specs=in_specs, out_specs=out_specs, check_vma=False
    )
```

```python
import functools
import math

import jax
import jax.numpy as jnp
import numpy as np
from jax import lax
from jax.experimental import pallas as pl
from jax.experimental.pallas import tpu as pltpu
from jax.sharding import Mesh
from jax.sharding import PartitionSpec as P

ORDER = 10
AZIM = 64
POLAR = 128
COEFS = 240
HALF = 120
FIELDS = 512
ROWS = 256
CHUNK = 32
LANES = 128
SPH_ANG = ("sph_0", "sph_1", "ang_0", "ang_1")
SPH = ("sph_0", "sph_1")
ANG = ("ang_0", "ang_1")
PLANE = ("ang_0", "sph_0")
LINE = "sph_1"
PAIR = "ang_1"
F32 = jnp.float32
BF16 = jnp.bfloat16


def index_tables():
    degree, order = np.zeros(LANES), np.zeros(LANES)
    for n in range(1, ORDER + 1):
        for m in range(-n, n + 1):
            degree[n * n - 1 + n + m] = n
            order[n * n - 1 + n + m] = m
    size = np.abs(order)
    used = degree > 0
    rise, fall = np.zeros((ORDER + 1, LANES)), np.zeros((ORDER + 1, LANES))
    for t in range(1, ORDER + 1):
        on = used & (size < t) & (t <= degree)
        s = size[on]
        rise[t, on] = np.sqrt((4.0 * t * t - 1.0) / (t * t - s * s))
        if t > 1:
            fall[t, on] = np.sqrt(((t - 1.0) ** 2 - s * s) / (4.0 * (t - 1.0) ** 2 - 1.0))
    link = np.sqrt((2 * degree + 1) * (degree**2 - order**2) / np.maximum(2 * degree - 1, 1)) * used
    norm = used / np.sqrt(np.maximum(degree * (degree + 1.0), 1.0))
    unit = np.array([1.0, -1.0j, -1.0, 1.0j])[(degree.astype(int) + 1) % 4] * norm
    return degree, order, size, rise, fall, link, unit


def constants():
    degree, order, size, rise, fall, link, unit = index_tables()
    rows = [order, degree, size, link, unit.real, unit.imag, 0 * size, 0 * size]
    table = np.zeros((32, LANES), np.float32)
    table[:8] = np.stack(rows)
    table[8 : 8 + ORDER] = rise[1:]
    table[20 : 20 + ORDER] = fall[1:]
    return table


def radial(const_ref, theta):
    order, degree, size, link = (const_ref[r : r + 1] for r in range(4))
    cos_theta, sine_theta = jnp.cos(theta), jnp.sin(theta)
    current = jnp.full(theta.shape, 1.0 / math.sqrt(4.0 * math.pi), F32)
    for t in range(1, ORDER + 1):
        factor = -math.sqrt((2.0 * t + 1.0) / (2.0 * t))
        current = jnp.where(size >= t, factor * sine_theta * current, current)
    previous = jnp.zeros_like(current)
    for t in range(1, ORDER + 1):
        rise, fall = const_ref[7 + t : 8 + t], const_ref[19 + t : 20 + t]
        following = rise * (cos_theta * current - fall * previous)
        previous = jnp.where(rise > 0, current, previous)
        current = jnp.where(rise > 0, following, current)
    pi_term = order * current / sine_theta
    tau_term = (degree * cos_theta * current - link * previous) / sine_theta
    return tau_term + pi_term, tau_term - pi_term, sine_theta


def halves(value):
    high = value.astype(BF16)
    return high, (value - high.astype(F32)).astype(BF16)


def swap_chunks(blocks):
    group = lax.broadcasted_iota(jnp.int32, blocks[0].shape, 1) // CHUNK
    out = []
    for x in range(4):
        mixed = None
        for g in range(4):
            shift = (g - x) * CHUNK % LANES
            piece = pltpu.roll(blocks[g], shift, 1) if shift else blocks[g]
            mixed = piece if mixed is None else jnp.where(group == g, piece, mixed)
        out.append(mixed)
    return out


def call(body, outs, ins, flops=1, limit=16, **kw):
    size = sum(math.prod(a.shape) * a.dtype.itemsize for a in list(outs) + list(ins))
    return pl.pallas_call(
        body,
        out_shape=[jax.ShapeDtypeStruct(o.shape, o.dtype) for o in outs],
        compiler_params=pltpu.CompilerParams(vmem_limit_bytes=limit * 1024 * 1024),
        cost_estimate=pl.CostEstimate(flops=flops, bytes_accessed=size, transcendentals=0),
        **kw,
    )(*ins)


def struct(shape, dtype=F32):
    return jax.ShapeDtypeStruct(shape, dtype)


def pack(total, part, out_ref):
    for tile in range(4):
        lanes = slice(tile * LANES, (tile + 1) * LANES)
        blocks = [total[part, g * 64 : (g + 1) * 64, lanes] for g in range(4)]
        for x, block in enumerate(swap_chunks(blocks)):
            out_ref[4 * tile + x] = block


def pack_kernel(core_ref, total_ref, detector_ref, out_ref):
    pack(total_ref, core_ref[0], out_ref)
    detector = detector_ref[...]
    detector = jnp.concatenate([detector[:, :CHUNK], detector[:, CHUNK:]], axis=0)
    for k in range(16):
        out_ref[k, 56:, 96:] = detector


def move_kernel(
    unroll, core_ref, cell_ref, coef_hbm, table_hbm, weight_ref, total, theirs_ref,
    coef, table, absorbed, right, sems,
):
    spheres = coef.shape[0]
    groups = spheres // unroll

    def coef_copy(j):
        return pltpu.make_async_copy(coef_hbm.at[j], coef.at[j], sems.at[3, j])

    def table_copy(j, stage):
        axis = 2 - stage
        return pltpu.make_async_copy(
            table_hbm.at[axis, cell_ref[axis, j]], table.at[stage, j], sems.at[stage, j]
        )

    def fetches(group):
        own = range(group * unroll, (group + 1) * unroll)
        first = [copy for j in own for copy in (coef_copy(j), table_copy(j, 0))]
        return first, [table_copy(j, stage) for stage in (1, 2) for j in own]

    first, second = fetches(0)
    for copy in first + second:
        copy.start()
    total[...] = jnp.zeros_like(total)
    absorbed[...] = jnp.zeros_like(absorbed)
    weights = weight_ref[...].T
    for group in range(groups):
        for copy in first if group == 0 else first + second:
            copy.wait()
        if group + 1 < groups:
            ahead = fetches(group + 1)
            for copy in ahead[0] + ahead[1]:
                copy.start()
        for s in range(unroll):
            j = group * unroll + s
            real, imag = coef[j, :, :FIELDS].astype(F32), coef[j, :, FIELDS:].astype(F32)
            energy = (real * real + imag * imag) * weights[:, j : j + 1]
            absorbed[...] += jnp.sum(energy.reshape(COEFS // 8, 8, FIELDS), axis=0)
        for stage in range(3):
            if group == 0 and stage == 1:
                for copy in second:
                    copy.wait()
            for s in range(unroll):
                j = group * unroll + s
                matrix = table[stage, j]
                turned = jnp.concatenate([-matrix[COEFS:], matrix[:COEFS]], axis=0)
                if stage == 0:
                    real, imag = coef[j, :, :FIELDS], coef[j, :, FIELDS:]
                else:
                    real, imag = right[s, :COEFS], right[s, ROWS : ROWS + COEFS]
                product = jnp.dot(matrix, real, preferred_element_type=F32) + jnp.dot(
                    turned, imag, preferred_element_type=F32
                )
                if stage < 2:
                    product = product.astype(BF16)
                    right[s, :COEFS] = product[:COEFS]
                    right[s, ROWS : ROWS + COEFS] = product[COEFS:]
                else:
                    total[0, :COEFS] += product[:COEFS]
                    total[1, :COEFS] += product[COEFS:]
        if group + 1 < groups:
            first, second = ahead
    total[0, COEFS : COEFS + 1] = jnp.sum(absorbed[...], axis=0, keepdims=True)
    pack(total, 1 - core_ref[0], theirs_ref)


def moved_sum(coefficients, positions, shift_tables, absorb_weight, core, unroll=2):
    spheres = coefficients.shape[0]
    smem = pl.BlockSpec(memory_space=pltpu.SMEM)
    hbm = pl.BlockSpec(memory_space=pltpu.HBM)
    vmem = pl.BlockSpec(memory_space=pltpu.VMEM)
    return pl.pallas_call(
        functools.partial(move_kernel, unroll),
        in_specs=[smem, smem, hbm, hbm, vmem],
        out_specs=[vmem, vmem],
        scratch_shapes=[
            pltpu.VMEM((spheres, COEFS, 2 * FIELDS), BF16),
            pltpu.VMEM((3, spheres, 2 * COEFS, COEFS), BF16),
            pltpu.VMEM((8, FIELDS), F32),
            pltpu.VMEM((unroll, 2 * ROWS, FIELDS), BF16),
            pltpu.SemaphoreType.DMA((4, spheres)),
        ],
        out_shape=[struct((2, ROWS, FIELDS)), struct((16, 64, LANES))],
        compiler_params=pltpu.CompilerParams(vmem_limit_bytes=52 * 1024 * 1024),
        cost_estimate=pl.CostEstimate(
            flops=6_000_000_000, bytes_accessed=10_000_000, transcendentals=0
        ),
        name="move",
    )(core, positions.T, coefficients, shift_tables, absorb_weight)


def plane_kernel(got_ref, out_ref):
    total = got_ref[0]
    for k in range(1, 16):
        total = total + got_ref[k]
    group = lax.broadcasted_iota(jnp.int32, (8, LANES), 1) // CHUNK
    detectors = got_ref[3, 56:]
    for x in range(3):
        detectors = jnp.where(
            group == x, pltpu.roll(got_ref[x, 56:], (x + 1) * CHUNK, 1), detectors
        )
    for k in range(8):
        out_ref[k, :64] = total
        out_ref[k, 64:] = detectors


def tables_kernel(
    place_ref, const_ref, high_ref, low_ref, turned_ref, fixed_ref, gap_ref, waves_ref, phase_ref
):
    z, core = place_ref[0], place_ref[1]
    row = lambda shape: lax.broadcasted_iota(jnp.int32, shape, 0)
    step = math.pi / POLAR

    near = row((16, LANES))
    near = ((near // 4) * 8 + z) * 4 + near % 4
    plus, minus, _ = radial(const_ref, (near.astype(F32) + 0.5) * step)
    azim = row((32, LANES))
    azim = ((azim // 8) * 2 + core) * 8 + azim % 8
    turn = (azim * const_ref[0:1].astype(jnp.int32)) & (AZIM - 1)
    angle = turn.astype(F32) * (2.0 * math.pi / AZIM)
    for sign, table in enumerate((plus, minus)):
        for trig, wave in enumerate((jnp.cos(angle), jnp.sin(angle))):
            block = table[None, :, None, :] * wave.reshape(4, 1, 8, LANES)
            high, low = halves(block.reshape(2 * ROWS, LANES))
            lanes = slice((2 * sign + trig) * LANES, (2 * sign + trig + 1) * LANES)
            high_ref[:, lanes] = high
            low_ref[:, lanes] = low

    plus, minus, sine_theta = radial(
        const_ref, (row((POLAR, LANES)).astype(F32) + 0.5) * step
    )
    weight = sine_theta * (2.0 * math.pi * math.pi / (POLAR * AZIM))
    for sign, table in enumerate((plus, minus)):
        turned_ref[sign] = (table * weight).T
        high, low = halves(table)
        for block in range(2):
            fixed_ref[sign, block * LANES : (block + 1) * LANES, :LANES] = high
            fixed_ref[sign, block * LANES : (block + 1) * LANES, LANES:] = low

    across = lambda r: jnp.broadcast_to(const_ref[r : r + 1], (LANES, LANES))
    used = across(1) > 0
    order = across(0)
    gap = jnp.where(used, order, 200.0) - jnp.where(used, order, 100.0).T
    gap_ref[...] = gap
    phase_ref[0] = across(4).T
    phase_ref[1] = across(5).T

    shape = (LANES, LANES)
    lane = lax.broadcasted_iota(jnp.int32, shape, 1)
    for half in range(2):
        azim = row(shape) % CHUNK + half * CHUNK
        turn = (azim * (lane % 64) - jnp.where(lane < 64, 0, AZIM // 4)) & (AZIM - 1)
        wave = jnp.cos(turn.astype(F32) * (2.0 * math.pi / AZIM))
        waves_ref[:, half * LANES : (half + 1) * LANES] = wave


def power_kernel(turned_ref, fixed_ref, line_ref, waves_ref, gap_ref, out_ref):
    gap = gap_ref[...]
    detectors = line_ref[:, 64:].reshape(64, LANES)
    group = lax.broadcasted_iota(jnp.int32, detectors.shape, 1) // CHUNK
    detectors = jnp.concatenate([jnp.where(group == x, detectors, 0.0) for x in range(4)], axis=0)
    spectrum = jnp.dot(
        detectors, waves_ref[...], preferred_element_type=F32, precision=lax.Precision.HIGHEST
    )
    spectrum = spectrum[:, :LANES] + pltpu.roll(spectrum[:, LANES:], 2 * LANES - 4, 0)
    spectrum = jnp.concatenate([spectrum[8 * k : 8 * k + 4] for k in range(32)], axis=0)
    spectrum = spectrum.T
    far = jnp.abs(gap[:HALF])
    far = jnp.concatenate([far, far], axis=0)
    for sign in range(2):
        table = turned_ref[sign, :HALF]
        fixed = fixed_ref[sign]
        total = jnp.zeros((COEFS, LANES), F32)
        for start in range(0, 2 * ORDER + 1, 7):
            rows = []
            for d in range(start, start + 7):
                rows += [table * spectrum[d : d + 1], table * spectrum[64 + d : 65 + d]]
            high, low = halves(jnp.concatenate(rows, axis=0))
            product = jnp.dot(
                jnp.concatenate([high, low], axis=1), fixed, preferred_element_type=F32
            )
            product = product[:, :LANES] + product[:, LANES:]
            for k in range(7):
                part = product[k * COEFS : (k + 1) * COEFS]
                total = jnp.where(far == start + k, part, total)
        out_ref[sign, 0, :HALF] = total[:HALF]
        out_ref[sign, 1, :HALF] = jnp.where(gap[:HALF] < 0, -total[HALF:], total[HALF:])
        out_ref[sign, :, HALF:] = jnp.zeros((2, 8, LANES), F32)


def spread_rows(packed):
    parts = [packed] + [pltpu.roll(packed, LANES - g * CHUNK, 1) for g in (1, 2, 3)]
    return jnp.concatenate(parts, axis=0)


def columns(group, pieces):
    out = pieces[0]
    for g in (1, 2, 3):
        out = jnp.where(group == g, pltpu.roll(pieces[g], g * CHUNK, 1), out)
    return out


def far_kernel(
    core_ref, own_ref, other_ref, high_ref, low_ref, form_ref, phase_ref,
    incident_ref, incident_imag_ref, out_ref,
):
    core = core_ref[0]
    own, other = own_ref[...], other_ref[...]
    real = spread_rows(jnp.where(core == 0, own, other))
    imag = spread_rows(jnp.where(core == 0, other, own))
    group = lax.broadcasted_iota(jnp.int32, (HALF, LANES), 1) // CHUNK
    spare = jnp.zeros((8, LANES), F32)
    phase_real, phase_imag = phase_ref[0, :HALF], phase_ref[1, :HALF]
    real_1, real_2 = real[:HALF], real[HALF:COEFS]
    imag_1, imag_2 = imag[:HALF], imag[HALF:COEFS]
    rows = []
    collected = jnp.zeros((1, LANES), F32)
    for sign in range(2):
        if sign == 0:
            both = (real_2 - imag_1, imag_2 + real_1)
        else:
            both = (real_2 + imag_1, imag_2 - real_1)
        re = phase_real * both[0] - phase_imag * both[1]
        im = phase_real * both[1] + phase_imag * both[0]
        if sign == 0:
            top = columns(group, (re, im, -im, re))
            low = columns(group, (-im, re, -re, -im))
        else:
            top = columns(group, (re, im, im, -re))
            low = columns(group, (-im, re, re, im))
        rows += [0.5 * top, spare, 0.5 * low, spare]
        pair = jnp.concatenate([jnp.where(group == 0, re, 0.0), spare], axis=0)
        pair_imag = jnp.concatenate([jnp.where(group == 0, im, 0.0), spare], axis=0)
        dot = functools.partial(
            jnp.dot, preferred_element_type=F32, precision=lax.Precision.HIGHEST
        )
        even, odd = form_ref[sign, 0], form_ref[sign, 1]
        collected += 0.5 * jnp.sum(
            pair * dot(even, pair)
            + pair_imag * (dot(even, pair_imag) + 2.0 * dot(odd, pair)),
            axis=0,
            keepdims=True,
        )
    high, low = halves(jnp.concatenate(rows, axis=0))
    wide = jnp.dot(
        high_ref[...], jnp.concatenate([high, low], axis=1), preferred_element_type=F32
    )
    result = (
        wide[:, :LANES]
        + wide[:, LANES:]
        + jnp.dot(low_ref[...], high, preferred_element_type=F32)
    )
    extinction = jnp.sum(
        incident_ref[...] * real[:COEFS, :CHUNK] + incident_imag_ref[...] * imag[:COEFS, :CHUNK],
        axis=0,
        keepdims=True,
    )
    stats = jnp.concatenate(
        [
            extinction,
            real[COEFS : COEFS + 1, :CHUNK],
            collected[:, :CHUNK],
            jnp.zeros((1, CHUNK), F32),
        ],
        axis=1,
    )
    stats = jnp.broadcast_to(stats, (8, LANES))
    for k in range(16):
        out_ref[k, :CHUNK] = result[k * CHUNK : (k + 1) * CHUNK]
        out_ref[k, CHUNK:] = stats


def finish_kernel(place_ref, got_ref, amplitude_ref, stats_ref):
    for tile in range(4):
        blocks = [got_ref[4 * tile + x, :CHUNK] for x in range(4)]
        for q, block in enumerate(swap_chunks(blocks)):
            amplitude_ref[q, :, tile * LANES : (tile + 1) * LANES] = block
    place = place_ref[0]
    first = got_ref[place, CHUNK : CHUNK + 1]
    second = got_ref[place + 1, CHUNK : CHUNK + 1]
    stats_ref[...] = jnp.concatenate(
        [
            jnp.concatenate(
                [v[:, r * CHUNK : (r + 1) * CHUNK] for v in (first, second)], axis=1
            )
            for r in range(3)
        ],
        axis=0,
    )


def shards(coefficients, positions, shift_tables, absorb_weight, incident, detector):
    x, z = lax.axis_index("sph_0"), lax.axis_index("sph_1")
    y, core = lax.axis_index("ang_0"), lax.axis_index("ang_1")
    smem = pl.BlockSpec(memory_space=pltpu.SMEM)
    vmem = pl.BlockSpec(memory_space=pltpu.VMEM)

    total, theirs = moved_sum(
        coefficients, positions, shift_tables, absorb_weight, core.reshape(1)
    )
    other = lax.ppermute(theirs, PAIR, [(0, 1), (1, 0)])
    (mine,) = call(
        pack_kernel,
        [struct((16, 64, LANES))],
        [core.reshape(1), total, detector],
        flops=10_000_000,
        in_specs=[smem, vmem, vmem],
    )
    packed = mine + other
    packed, incident, x, z, y, core = lax.optimization_barrier(
        (packed, incident, x, z, y, core)
    )
    high, low, turned, fixed, gap, waves, phase = call(
        tables_kernel,
        [
            struct((2 * ROWS, 2 * ROWS), BF16), struct((2 * ROWS, 2 * ROWS), BF16),
            struct((2, LANES, POLAR)), struct((2, 2 * POLAR, 2 * LANES), BF16), struct((LANES, LANES)),
            struct((LANES, 2 * LANES)), struct((2, LANES, LANES)),
        ],
        [jnp.stack([z, core]), jnp.asarray(constants())],
        flops=100_000_000,
        in_specs=[smem, vmem],
    )
    first = (4 * y + x) * CHUNK
    tables = (
        turned, fixed, waves, gap, high, low, phase,
        lax.dynamic_slice_in_dim(incident, first, CHUNK, 1),
        lax.dynamic_slice_in_dim(incident, FIELDS + first, CHUNK, 1),
        core.astype(jnp.int32).reshape(1), (4 * y + 2 * core).astype(jnp.int32).reshape(1),
    )
    got = lax.all_to_all(packed, PLANE, 0, 0, tiled=True)
    got, tables = lax.optimization_barrier((got, tables))
    turned, fixed, waves, gap, high, low, phase, inc_real, inc_imag, core, place = tables
    (spread,) = call(plane_kernel, [struct((8, 72, LANES))], [got])
    line = lax.all_to_all(spread, LINE, 0, 0, tiled=True)
    own = line[:, :64].sum(axis=0)
    partner = lax.ppermute(own, PAIR, [(0, 1), (1, 0)])
    (form,) = call(
        power_kernel,
        [struct((2, 2, LANES, LANES))],
        [turned, fixed, line, waves, gap],
        flops=1_000_000_000,
    )
    (messages,) = call(
        far_kernel,
        [struct((16, 40, LANES))],
        [core, own, partner, high, low, form, phase, inc_real, inc_imag],
        flops=400_000_000,
        in_specs=[smem] + [vmem] * 8,
    )
    got = lax.all_to_all(messages, PLANE, 0, 0, tiled=True)
    amplitude, stats = call(
        finish_kernel,
        [struct((4, 32, FIELDS)), struct((3, 64))],
        [place, got],
        in_specs=[smem, vmem],
    )
    return (amplitude.reshape(2, 2, 4, 8, FIELDS), stats)


def solution(mesh):
    torus = Mesh(mesh.devices.reshape(4, 8, 4, 2), SPH_ANG)
    in_specs = (P(SPH_ANG, None, None), P(SPH_ANG, None), P(), P(SPH_ANG, None), P(), P(SPH, None))
    out_specs = (P(None, None, SPH, ANG, None), P(None, ANG))
    return jax.shard_map(
        shards, mesh=torus, in_specs=in_specs, out_specs=out_specs, check_vma=False
    )
```

```python
import functools
import math

import jax
import jax.numpy as jnp
import numpy as np
from jax import lax
from jax.experimental import pallas as pl
from jax.experimental.pallas import tpu as pltpu
from jax.sharding import Mesh
from jax.sharding import PartitionSpec as P

ORDER = 10
AZIM = 64
POLAR = 128
COEFS = 240
HALF = 120
FIELDS = 512
ROWS = 256
CHUNK = 32
LANES = 128
SPH_ANG = ("sph_0", "sph_1", "ang_0", "ang_1")
SPH = ("sph_0", "sph_1")
ANG = ("ang_0", "ang_1")
PLANE = ("ang_0", "sph_0")
LINE = "sph_1"
PAIR = "ang_1"
F32 = jnp.float32
BF16 = jnp.bfloat16


def index_tables():
    degree, order = np.zeros(LANES), np.zeros(LANES)
    for n in range(1, ORDER + 1):
        for m in range(-n, n + 1):
            degree[n * n - 1 + n + m] = n
            order[n * n - 1 + n + m] = m
    size = np.abs(order)
    used = degree > 0
    rise, fall = np.zeros((ORDER + 1, LANES)), np.zeros((ORDER + 1, LANES))
    for t in range(1, ORDER + 1):
        on = used & (size < t) & (t <= degree)
        s = size[on]
        rise[t, on] = np.sqrt((4.0 * t * t - 1.0) / (t * t - s * s))
        if t > 1:
            fall[t, on] = np.sqrt(((t - 1.0) ** 2 - s * s) / (4.0 * (t - 1.0) ** 2 - 1.0))
    link = np.sqrt((2 * degree + 1) * (degree**2 - order**2) / np.maximum(2 * degree - 1, 1)) * used
    norm = used / np.sqrt(np.maximum(degree * (degree + 1.0), 1.0))
    unit = np.array([1.0, -1.0j, -1.0, 1.0j])[(degree.astype(int) + 1) % 4] * norm
    return degree, order, size, rise, fall, link, unit


def constants():
    degree, order, size, rise, fall, link, unit = index_tables()
    rows = [order, degree, size, link, unit.real, unit.imag, 0 * size, 0 * size]
    table = np.zeros((32, LANES), np.float32)
    table[:8] = np.stack(rows)
    table[8 : 8 + ORDER] = rise[1:]
    table[20 : 20 + ORDER] = fall[1:]
    return table


def radial(const_ref, theta):
    order, degree, size, link = (const_ref[r : r + 1] for r in range(4))
    cos_theta, sine_theta = jnp.cos(theta), jnp.sin(theta)
    current = jnp.full(theta.shape, 1.0 / math.sqrt(4.0 * math.pi), F32)
    for t in range(1, ORDER + 1):
        factor = -math.sqrt((2.0 * t + 1.0) / (2.0 * t))
        current = jnp.where(size >= t, factor * sine_theta * current, current)
    previous = jnp.zeros_like(current)
    for t in range(1, ORDER + 1):
        rise, fall = const_ref[7 + t : 8 + t], const_ref[19 + t : 20 + t]
        following = rise * (cos_theta * current - fall * previous)
        previous = jnp.where(rise > 0, current, previous)
        current = jnp.where(rise > 0, following, current)
    pi_term = order * current / sine_theta
    tau_term = (degree * cos_theta * current - link * previous) / sine_theta
    return tau_term + pi_term, tau_term - pi_term, sine_theta


def halves(value):
    high = value.astype(BF16)
    return high, (value - high.astype(F32)).astype(BF16)


def swap_chunks(blocks):
    group = lax.broadcasted_iota(jnp.int32, blocks[0].shape, 1) // CHUNK
    out = []
    for x in range(4):
        mixed = None
        for g in range(4):
            shift = (g - x) * CHUNK % LANES
            piece = pltpu.roll(blocks[g], shift, 1) if shift else blocks[g]
            mixed = piece if mixed is None else jnp.where(group == g, piece, mixed)
        out.append(mixed)
    return out


def call(body, outs, ins, flops=1, limit=16, **kw):
    size = sum(math.prod(a.shape) * a.dtype.itemsize for a in list(outs) + list(ins))
    return pl.pallas_call(
        body,
        out_shape=[jax.ShapeDtypeStruct(o.shape, o.dtype) for o in outs],
        compiler_params=pltpu.CompilerParams(vmem_limit_bytes=limit * 1024 * 1024),
        cost_estimate=pl.CostEstimate(flops=flops, bytes_accessed=size, transcendentals=0),
        **kw,
    )(*ins)


def struct(shape, dtype=F32):
    return jax.ShapeDtypeStruct(shape, dtype)


def pack(total, part, out_ref):
    for tile in range(4):
        lanes = slice(tile * LANES, (tile + 1) * LANES)
        blocks = [total[part, g * 64 : (g + 1) * 64, lanes] for g in range(4)]
        for x, block in enumerate(swap_chunks(blocks)):
            out_ref[4 * tile + x] = block


def pack_kernel(core_ref, total_ref, detector_ref, out_ref):
    pack(total_ref, core_ref[0], out_ref)
    detector = detector_ref[...]
    detector = jnp.concatenate([detector[:, :CHUNK], detector[:, CHUNK:]], axis=0)
    for k in range(16):
        out_ref[k, 56:, 96:] = detector


def move_kernel(
    unroll, core_ref, coef_hbm, table_hbm, weight_ref, total, theirs_ref,
    coef, table, absorbed, right, cell_ref, sems, cell_sem,
):
    spheres = coef.shape[0]
    groups = spheres // unroll

    def coef_copy(j):
        return pltpu.make_async_copy(coef_hbm.at[j], coef.at[j], sems.at[3, j])

    def table_copy(j, stage):
        axis = 2 - stage
        return pltpu.make_async_copy(
            table_hbm.at[axis, cell_ref[spheres + axis, j].astype(jnp.int32)],
            table.at[stage, j],
            sems.at[stage, j],
        )

    def fetches(group):
        own = range(group * unroll, (group + 1) * unroll)
        first = [copy for j in own for copy in (coef_copy(j), table_copy(j, 0))]
        return first, [table_copy(j, stage) for stage in (1, 2) for j in own]

    for j in range(unroll):
        coef_copy(j).start()
    cells = pltpu.make_async_copy(weight_ref, cell_ref, cell_sem)
    cells.start()
    cells.wait()
    first, second = fetches(0)
    for copy in first[1::2] + second:
        copy.start()
    total[...] = jnp.zeros_like(total)
    absorbed[...] = jnp.zeros_like(absorbed)
    weights = weight_ref[:spheres].T[:COEFS]
    for group in range(groups):
        for copy in first if group == 0 else first + second:
            copy.wait()
        if group + 1 < groups:
            ahead = fetches(group + 1)
            for copy in ahead[0] + ahead[1]:
                copy.start()
        for s in range(unroll):
            j = group * unroll + s
            real, imag = coef[j, :, :FIELDS].astype(F32), coef[j, :, FIELDS:].astype(F32)
            energy = (real * real + imag * imag) * weights[:, j : j + 1]
            absorbed[...] += jnp.sum(energy.reshape(COEFS // 8, 8, FIELDS), axis=0)
        for stage in range(3):
            if group == 0 and stage == 1:
                for copy in second:
                    copy.wait()
            for s in range(unroll):
                j = group * unroll + s
                matrix = table[stage, j]
                turned = jnp.concatenate([-matrix[COEFS:], matrix[:COEFS]], axis=0)
                if stage == 0:
                    real, imag = coef[j, :, :FIELDS], coef[j, :, FIELDS:]
                else:
                    real, imag = right[s, :COEFS], right[s, ROWS : ROWS + COEFS]
                product = jnp.dot(matrix, real, preferred_element_type=F32) + jnp.dot(
                    turned, imag, preferred_element_type=F32
                )
                if stage < 2:
                    product = product.astype(BF16)
                    right[s, :COEFS] = product[:COEFS]
                    right[s, ROWS : ROWS + COEFS] = product[COEFS:]
                else:
                    total[0, :COEFS] += product[:COEFS]
                    total[1, :COEFS] += product[COEFS:]
        if group + 1 < groups:
            first, second = ahead
    total[0, COEFS : COEFS + 1] = jnp.sum(absorbed[...], axis=0, keepdims=True)
    pack(total, 1 - core_ref[0], theirs_ref)


def moved_sum(coefficients, positions, shift_tables, absorb_weight, core, unroll=2):
    spheres = coefficients.shape[0]
    smem = pl.BlockSpec(memory_space=pltpu.SMEM)
    cells = positions.T.astype(F32)
    weights = jnp.concatenate(
        [
            jnp.pad(absorb_weight, ((0, 0), (0, ROWS - COEFS))),
            jnp.pad(cells, ((0, 8 - cells.shape[0]), (0, ROWS - spheres))),
        ],
        axis=0,
    )
    hbm = pl.BlockSpec(memory_space=pltpu.HBM)
    vmem = pl.BlockSpec(memory_space=pltpu.VMEM)
    return pl.pallas_call(
        functools.partial(move_kernel, unroll),
        in_specs=[smem, hbm, hbm, vmem],
        out_specs=[vmem, vmem],
        scratch_shapes=[
            pltpu.VMEM((spheres, COEFS, 2 * FIELDS), BF16),
            pltpu.VMEM((3, spheres, 2 * COEFS, COEFS), BF16),
            pltpu.VMEM((8, FIELDS), F32),
            pltpu.VMEM((unroll, 2 * ROWS, FIELDS), BF16),
            pltpu.SMEM((spheres + 8, ROWS), F32),
            pltpu.SemaphoreType.DMA((4, spheres)),
            pltpu.SemaphoreType.DMA,
        ],
        out_shape=[struct((2, ROWS, FIELDS)), struct((16, 64, LANES))],
        compiler_params=pltpu.CompilerParams(vmem_limit_bytes=52 * 1024 * 1024),
        cost_estimate=pl.CostEstimate(
            flops=6_000_000_000, bytes_accessed=10_000_000, transcendentals=0
        ),
        name="move",
    )(core, coefficients, shift_tables, weights)


def plane_kernel(got_ref, out_ref):
    total = got_ref[0]
    for k in range(1, 16):
        total = total + got_ref[k]
    group = lax.broadcasted_iota(jnp.int32, (8, LANES), 1) // CHUNK
    detectors = got_ref[3, 56:]
    for x in range(3):
        detectors = jnp.where(
            group == x, pltpu.roll(got_ref[x, 56:], (x + 1) * CHUNK, 1), detectors
        )
    for k in range(8):
        out_ref[k, :64] = total
        out_ref[k, 64:] = detectors


def tables_kernel(
    place_ref, const_ref, high_ref, low_ref, turned_ref, fixed_ref, gap_ref, waves_ref, phase_ref
):
    z, core = place_ref[0], place_ref[1]
    row = lambda shape: lax.broadcasted_iota(jnp.int32, shape, 0)
    step = math.pi / POLAR

    near = row((16, LANES))
    near = ((near // 4) * 8 + z) * 4 + near % 4
    plus, minus, _ = radial(const_ref, (near.astype(F32) + 0.5) * step)
    azim = row((32, LANES))
    azim = ((azim // 8) * 2 + core) * 8 + azim % 8
    turn = (azim * const_ref[0:1].astype(jnp.int32)) & (AZIM - 1)
    angle = turn.astype(F32) * (2.0 * math.pi / AZIM)
    for sign, table in enumerate((plus, minus)):
        for trig, wave in enumerate((jnp.cos(angle), jnp.sin(angle))):
            block = table[None, :, None, :] * wave.reshape(4, 1, 8, LANES)
            high, low = halves(block.reshape(2 * ROWS, LANES))
            lanes = slice((2 * sign + trig) * LANES, (2 * sign + trig + 1) * LANES)
            high_ref[:, lanes] = high
            low_ref[:, lanes] = low

    plus, minus, sine_theta = radial(
        const_ref, (row((POLAR, LANES)).astype(F32) + 0.5) * step
    )
    weight = sine_theta * (2.0 * math.pi * math.pi / (POLAR * AZIM))
    for sign, table in enumerate((plus, minus)):
        turned_ref[sign] = (table * weight).T
        high, low = halves(table)
        for block in range(2):
            fixed_ref[sign, block * LANES : (block + 1) * LANES, :LANES] = high
            fixed_ref[sign, block * LANES : (block + 1) * LANES, LANES:] = low

    across = lambda r: jnp.broadcast_to(const_ref[r : r + 1], (LANES, LANES))
    used = across(1) > 0
    order = across(0)
    gap = jnp.where(used, order, 200.0) - jnp.where(used, order, 100.0).T
    gap_ref[...] = gap
    phase_ref[0] = across(4).T
    phase_ref[1] = across(5).T

    shape = (LANES, LANES)
    lane = lax.broadcasted_iota(jnp.int32, shape, 1)
    for half in range(2):
        azim = row(shape) % CHUNK + half * CHUNK
        turn = (azim * (lane % 64) - jnp.where(lane < 64, 0, AZIM // 4)) & (AZIM - 1)
        wave = jnp.cos(turn.astype(F32) * (2.0 * math.pi / AZIM))
        waves_ref[:, half * LANES : (half + 1) * LANES] = wave


def power_kernel(turned_ref, fixed_ref, line_ref, waves_ref, gap_ref, out_ref):
    gap = gap_ref[...]
    detectors = line_ref[:, 64:].reshape(64, LANES)
    group = lax.broadcasted_iota(jnp.int32, detectors.shape, 1) // CHUNK
    detectors = jnp.concatenate([jnp.where(group == x, detectors, 0.0) for x in range(4)], axis=0)
    spectrum = jnp.dot(
        detectors, waves_ref[...], preferred_element_type=F32, precision=lax.Precision.HIGHEST
    )
    spectrum = spectrum[:, :LANES] + pltpu.roll(spectrum[:, LANES:], 2 * LANES - 4, 0)
    spectrum = jnp.concatenate([spectrum[8 * k : 8 * k + 4] for k in range(32)], axis=0)
    spectrum = spectrum.T
    far = jnp.abs(gap[:HALF])
    far = jnp.concatenate([far, far], axis=0)
    for sign in range(2):
        table = turned_ref[sign, :HALF]
        fixed = fixed_ref[sign]
        total = jnp.zeros((COEFS, LANES), F32)
        for start in range(0, 2 * ORDER + 1, 7):
            rows = []
            for d in range(start, start + 7):
                rows += [table * spectrum[d : d + 1], table * spectrum[64 + d : 65 + d]]
            high, low = halves(jnp.concatenate(rows, axis=0))
            product = jnp.dot(
                jnp.concatenate([high, low], axis=1), fixed, preferred_element_type=F32
            )
            product = product[:, :LANES] + product[:, LANES:]
            for k in range(7):
                part = product[k * COEFS : (k + 1) * COEFS]
                total = jnp.where(far == start + k, part, total)
        out_ref[sign, 0, :HALF] = total[:HALF]
        out_ref[sign, 1, :HALF] = jnp.where(gap[:HALF] < 0, -total[HALF:], total[HALF:])
        out_ref[sign, :, HALF:] = jnp.zeros((2, 8, LANES), F32)


def spread_rows(packed):
    parts = [packed] + [pltpu.roll(packed, LANES - g * CHUNK, 1) for g in (1, 2, 3)]
    return jnp.concatenate(parts, axis=0)


def columns(group, pieces):
    out = pieces[0]
    for g in (1, 2, 3):
        out = jnp.where(group == g, pltpu.roll(pieces[g], g * CHUNK, 1), out)
    return out


def far_kernel(
    core_ref, own_ref, other_ref, high_ref, low_ref, form_ref, phase_ref,
    incident_ref, incident_imag_ref, out_ref,
):
    core = core_ref[0]
    own, other = own_ref[...], other_ref[...]
    real = spread_rows(jnp.where(core == 0, own, other))
    imag = spread_rows(jnp.where(core == 0, other, own))
    group = lax.broadcasted_iota(jnp.int32, (HALF, LANES), 1) // CHUNK
    spare = jnp.zeros((8, LANES), F32)
    phase_real, phase_imag = phase_ref[0, :HALF], phase_ref[1, :HALF]
    real_1, real_2 = real[:HALF], real[HALF:COEFS]
    imag_1, imag_2 = imag[:HALF], imag[HALF:COEFS]
    rows = []
    collected = jnp.zeros((1, LANES), F32)
    for sign in range(2):
        if sign == 0:
            both = (real_2 - imag_1, imag_2 + real_1)
        else:
            both = (real_2 + imag_1, imag_2 - real_1)
        re = phase_real * both[0] - phase_imag * both[1]
        im = phase_real * both[1] + phase_imag * both[0]
        if sign == 0:
            top = columns(group, (re, im, -im, re))
            low = columns(group, (-im, re, -re, -im))
        else:
            top = columns(group, (re, im, im, -re))
            low = columns(group, (-im, re, re, im))
        rows += [0.5 * top, spare, 0.5 * low, spare]
        pair = jnp.concatenate([jnp.where(group == 0, re, 0.0), spare], axis=0)
        pair_imag = jnp.concatenate([jnp.where(group == 0, im, 0.0), spare], axis=0)
        dot = functools.partial(
            jnp.dot, preferred_element_type=F32, precision=lax.Precision.HIGHEST
        )
        even, odd = form_ref[sign, 0], form_ref[sign, 1]
        collected += 0.5 * jnp.sum(
            pair * dot(even, pair)
            + pair_imag * (dot(even, pair_imag) + 2.0 * dot(odd, pair)),
            axis=0,
            keepdims=True,
        )
    high, low = halves(jnp.concatenate(rows, axis=0))
    wide = jnp.dot(
        high_ref[...], jnp.concatenate([high, low], axis=1), preferred_element_type=F32
    )
    result = (
        wide[:, :LANES]
        + wide[:, LANES:]
        + jnp.dot(low_ref[...], high, preferred_element_type=F32)
    )
    extinction = jnp.sum(
        incident_ref[...] * real[:COEFS, :CHUNK] + incident_imag_ref[...] * imag[:COEFS, :CHUNK],
        axis=0,
        keepdims=True,
    )
    stats = jnp.concatenate(
        [
            extinction,
            real[COEFS : COEFS + 1, :CHUNK],
            collected[:, :CHUNK],
            jnp.zeros((1, CHUNK), F32),
        ],
        axis=1,
    )
    stats = jnp.broadcast_to(stats, (8, LANES))
    for k in range(16):
        out_ref[k, :CHUNK] = result[k * CHUNK : (k + 1) * CHUNK]
        out_ref[k, CHUNK:] = stats


def finish_kernel(place_ref, got_ref, amplitude_ref, stats_ref):
    for tile in range(4):
        blocks = [got_ref[4 * tile + x, :CHUNK] for x in range(4)]
        for q, block in enumerate(swap_chunks(blocks)):
            amplitude_ref[q, :, tile * LANES : (tile + 1) * LANES] = block
    place = place_ref[0]
    first = got_ref[place, CHUNK : CHUNK + 1]
    second = got_ref[place + 1, CHUNK : CHUNK + 1]
    stats_ref[...] = jnp.concatenate(
        [
            jnp.concatenate(
                [v[:, r * CHUNK : (r + 1) * CHUNK] for v in (first, second)], axis=1
            )
            for r in range(3)
        ],
        axis=0,
    )


def shards(coefficients, positions, shift_tables, absorb_weight, incident, detector):
    x, z = lax.axis_index("sph_0"), lax.axis_index("sph_1")
    y, core = lax.axis_index("ang_0"), lax.axis_index("ang_1")
    smem = pl.BlockSpec(memory_space=pltpu.SMEM)
    vmem = pl.BlockSpec(memory_space=pltpu.VMEM)

    total, theirs = moved_sum(
        coefficients, positions, shift_tables, absorb_weight, core.reshape(1)
    )
    other = lax.ppermute(theirs, PAIR, [(0, 1), (1, 0)])
    (mine,) = call(
        pack_kernel,
        [struct((16, 64, LANES))],
        [core.reshape(1), total, detector],
        flops=10_000_000,
        in_specs=[smem, vmem, vmem],
    )
    packed = mine + other
    packed, incident, x, z, y, core = lax.optimization_barrier(
        (packed, incident, x, z, y, core)
    )
    high, low, turned, fixed, gap, waves, phase = call(
        tables_kernel,
        [
            struct((2 * ROWS, 2 * ROWS), BF16), struct((2 * ROWS, 2 * ROWS), BF16),
            struct((2, LANES, POLAR)), struct((2, 2 * POLAR, 2 * LANES), BF16), struct((LANES, LANES)),
            struct((LANES, 2 * LANES)), struct((2, LANES, LANES)),
        ],
        [jnp.stack([z, core]), jnp.asarray(constants())],
        flops=100_000_000,
        in_specs=[smem, vmem],
    )
    first = (4 * y + x) * CHUNK
    tables = (
        turned, fixed, waves, gap, high, low, phase,
        lax.dynamic_slice_in_dim(incident, first, CHUNK, 1),
        lax.dynamic_slice_in_dim(incident, FIELDS + first, CHUNK, 1),
        core.astype(jnp.int32).reshape(1), (4 * y + 2 * core).astype(jnp.int32).reshape(1),
    )
    got = lax.all_to_all(packed, PLANE, 0, 0, tiled=True)
    got, tables = lax.optimization_barrier((got, tables))
    turned, fixed, waves, gap, high, low, phase, inc_real, inc_imag, core, place = tables
    (spread,) = call(plane_kernel, [struct((8, 72, LANES))], [got])
    line = lax.all_to_all(spread, LINE, 0, 0, tiled=True)
    own = line[:, :64].sum(axis=0)
    partner = lax.ppermute(own, PAIR, [(0, 1), (1, 0)])
    (form,) = call(
        power_kernel,
        [struct((2, 2, LANES, LANES))],
        [turned, fixed, line, waves, gap],
        flops=1_000_000_000,
    )
    (messages,) = call(
        far_kernel,
        [struct((16, 40, LANES))],
        [core, own, partner, high, low, form, phase, inc_real, inc_imag],
        flops=400_000_000,
        in_specs=[smem] + [vmem] * 8,
    )
    got = lax.all_to_all(messages, PLANE, 0, 0, tiled=True)
    amplitude, stats = call(
        finish_kernel,
        [struct((4, 32, FIELDS)), struct((3, 64))],
        [place, got],
        in_specs=[smem, vmem],
    )
    return (amplitude.reshape(2, 2, 4, 8, FIELDS), stats)


def solution(mesh):
    torus = Mesh(mesh.devices.reshape(4, 8, 4, 2), SPH_ANG)
    in_specs = (P(SPH_ANG, None, None), P(SPH_ANG, None), P(), P(SPH_ANG, None), P(), P(SPH, None))
    out_specs = (P(None, None, SPH, ANG, None), P(None, ANG))
    return jax.shard_map(
        shards, mesh=torus, in_specs=in_specs, out_specs=out_specs, check_vma=False
    )
```

```python
import functools
import math

import jax
import jax.numpy as jnp
import numpy as np
from jax import lax
from jax.experimental import pallas as pl
from jax.experimental.pallas import tpu as pltpu
from jax.sharding import Mesh
from jax.sharding import PartitionSpec as P

ORDER = 10
AZIM = 64
POLAR = 128
COEFS = 240
HALF = 120
FIELDS = 512
ROWS = 256
CHUNK = 32
LANES = 128
SPH_ANG = ("sph_0", "sph_1", "ang_0", "ang_1")
SPH = ("sph_0", "sph_1")
ANG = ("ang_0", "ang_1")
PLANE = ("ang_0", "sph_0")
LINE = "sph_1"
PAIR = "ang_1"
F32 = jnp.float32
BF16 = jnp.bfloat16


def index_tables():
    degree, order = np.zeros(LANES), np.zeros(LANES)
    for n in range(1, ORDER + 1):
        for m in range(-n, n + 1):
            degree[n * n - 1 + n + m] = n
            order[n * n - 1 + n + m] = m
    size = np.abs(order)
    used = degree > 0
    rise, fall = np.zeros((ORDER + 1, LANES)), np.zeros((ORDER + 1, LANES))
    for t in range(1, ORDER + 1):
        on = used & (size < t) & (t <= degree)
        s = size[on]
        rise[t, on] = np.sqrt((4.0 * t * t - 1.0) / (t * t - s * s))
        if t > 1:
            fall[t, on] = np.sqrt(((t - 1.0) ** 2 - s * s) / (4.0 * (t - 1.0) ** 2 - 1.0))
    link = np.sqrt((2 * degree + 1) * (degree**2 - order**2) / np.maximum(2 * degree - 1, 1)) * used
    norm = used / np.sqrt(np.maximum(degree * (degree + 1.0), 1.0))
    unit = np.array([1.0, -1.0j, -1.0, 1.0j])[(degree.astype(int) + 1) % 4] * norm
    return degree, order, size, rise, fall, link, unit


def constants():
    degree, order, size, rise, fall, link, unit = index_tables()
    rows = [order, degree, size, link, unit.real, unit.imag, 0 * size, 0 * size]
    table = np.zeros((32, LANES), np.float32)
    table[:8] = np.stack(rows)
    table[8 : 8 + ORDER] = rise[1:]
    table[20 : 20 + ORDER] = fall[1:]
    return table


def radial(const_ref, theta):
    order, degree, size, link = (const_ref[r : r + 1] for r in range(4))
    cos_theta, sine_theta = jnp.cos(theta), jnp.sin(theta)
    current = jnp.full(theta.shape, 1.0 / math.sqrt(4.0 * math.pi), F32)
    for t in range(1, ORDER + 1):
        factor = -math.sqrt((2.0 * t + 1.0) / (2.0 * t))
        current = jnp.where(size >= t, factor * sine_theta * current, current)
    previous = jnp.zeros_like(current)
    for t in range(1, ORDER + 1):
        rise, fall = const_ref[7 + t : 8 + t], const_ref[19 + t : 20 + t]
        following = rise * (cos_theta * current - fall * previous)
        previous = jnp.where(rise > 0, current, previous)
        current = jnp.where(rise > 0, following, current)
    pi_term = order * current / sine_theta
    tau_term = (degree * cos_theta * current - link * previous) / sine_theta
    return tau_term + pi_term, tau_term - pi_term, sine_theta


def halves(value):
    high = value.astype(BF16)
    return high, (value - high.astype(F32)).astype(BF16)


def swap_chunks(blocks):
    group = lax.broadcasted_iota(jnp.int32, blocks[0].shape, 1) // CHUNK
    out = []
    for x in range(4):
        mixed = None
        for g in range(4):
            shift = (g - x) * CHUNK % LANES
            piece = pltpu.roll(blocks[g], shift, 1) if shift else blocks[g]
            mixed = piece if mixed is None else jnp.where(group == g, piece, mixed)
        out.append(mixed)
    return out


def call(body, outs, ins, flops=1, limit=16, **kw):
    size = sum(math.prod(a.shape) * a.dtype.itemsize for a in list(outs) + list(ins))
    return pl.pallas_call(
        body,
        out_shape=[jax.ShapeDtypeStruct(o.shape, o.dtype) for o in outs],
        compiler_params=pltpu.CompilerParams(vmem_limit_bytes=limit * 1024 * 1024),
        cost_estimate=pl.CostEstimate(flops=flops, bytes_accessed=size, transcendentals=0),
        **kw,
    )(*ins)


def struct(shape, dtype=F32):
    return jax.ShapeDtypeStruct(shape, dtype)


def pack(total, part, out_ref):
    for tile in range(4):
        lanes = slice(tile * LANES, (tile + 1) * LANES)
        blocks = [total[part, g * 64 : (g + 1) * 64, lanes] for g in range(4)]
        for x, block in enumerate(swap_chunks(blocks)):
            out_ref[4 * tile + x] = block


def pack_kernel(core_ref, total_ref, detector_ref, out_ref):
    pack(total_ref, core_ref[0], out_ref)
    detector = detector_ref[...]
    detector = jnp.concatenate([detector[:, :CHUNK], detector[:, CHUNK:]], axis=0)
    for k in range(16):
        out_ref[k, 56:, 96:] = detector


def move_kernel(
    unroll, core_ref, coef_hbm, table_hbm, weight_ref, total, theirs_ref,
    coef, table, absorbed, right, cell_ref, sems, cell_sem,
):
    spheres = coef.shape[0]
    groups = spheres // unroll

    def coef_copy(j):
        return pltpu.make_async_copy(coef_hbm.at[j], coef.at[j], sems.at[3, j])

    def table_copy(j, stage):
        axis = 2 - stage
        return pltpu.make_async_copy(
            table_hbm.at[axis, cell_ref[spheres + axis, j].astype(jnp.int32)],
            table.at[stage, j],
            sems.at[stage, j],
        )

    def fetches(group):
        own = range(group * unroll, (group + 1) * unroll)
        first = [copy for j in own for copy in (coef_copy(j), table_copy(j, 0))]
        return first, [table_copy(j, stage) for stage in (1, 2) for j in own]

    for j in range(unroll):
        coef_copy(j).start()
    cells = pltpu.make_async_copy(weight_ref, cell_ref, cell_sem)
    cells.start()
    cells.wait()
    first, second = fetches(0)
    for copy in first[1::2] + second:
        copy.start()
    total[...] = jnp.zeros_like(total)
    absorbed[...] = jnp.zeros_like(absorbed)
    weights = weight_ref[:spheres].T[:COEFS]
    for group in range(groups):
        for copy in first if group == 0 else first + second:
            copy.wait()
        if group + 1 < groups:
            ahead = fetches(group + 1)
            for copy in ahead[0] + ahead[1]:
                copy.start()
        for s in range(unroll):
            j = group * unroll + s
            real, imag = coef[j, :, :FIELDS].astype(F32), coef[j, :, FIELDS:].astype(F32)
            energy = (real * real + imag * imag) * weights[:, j : j + 1]
            absorbed[...] += jnp.sum(energy.reshape(COEFS // 8, 8, FIELDS), axis=0)
        for stage in range(3):
            if group == 0 and stage == 1:
                for copy in second:
                    copy.wait()
            for s in range(unroll):
                j = group * unroll + s
                matrix = table[stage, j]
                turned = jnp.concatenate([-matrix[COEFS:], matrix[:COEFS]], axis=0)
                if stage == 0:
                    real, imag = coef[j, :, :FIELDS], coef[j, :, FIELDS:]
                else:
                    real, imag = right[s, :COEFS], right[s, ROWS : ROWS + COEFS]
                product = jnp.dot(matrix, real, preferred_element_type=F32) + jnp.dot(
                    turned, imag, preferred_element_type=F32
                )
                if stage < 2:
                    product = product.astype(BF16)
                    right[s, :COEFS] = product[:COEFS]
                    right[s, ROWS : ROWS + COEFS] = product[COEFS:]
                else:
                    total[0, :COEFS] += product[:COEFS]
                    total[1, :COEFS] += product[COEFS:]
        if group + 1 < groups:
            first, second = ahead
    total[0, COEFS : COEFS + 1] = jnp.sum(absorbed[...], axis=0, keepdims=True)
    pack(total, 1 - core_ref[0], theirs_ref)


def moved_sum(coefficients, positions, shift_tables, absorb_weight, core, unroll=2):
    spheres = coefficients.shape[0]
    smem = pl.BlockSpec(memory_space=pltpu.SMEM)
    cells = positions.T.astype(F32)
    weights = jnp.concatenate(
        [
            jnp.pad(absorb_weight, ((0, 0), (0, ROWS - COEFS))),
            jnp.pad(cells, ((0, 8 - cells.shape[0]), (0, ROWS - spheres))),
        ],
        axis=0,
    )
    hbm = pl.BlockSpec(memory_space=pltpu.HBM)
    vmem = pl.BlockSpec(memory_space=pltpu.VMEM)
    return pl.pallas_call(
        functools.partial(move_kernel, unroll),
        in_specs=[smem, hbm, hbm, vmem],
        out_specs=[vmem, vmem],
        scratch_shapes=[
            pltpu.VMEM((spheres, COEFS, 2 * FIELDS), BF16),
            pltpu.VMEM((3, spheres, 2 * COEFS, COEFS), BF16),
            pltpu.VMEM((8, FIELDS), F32),
            pltpu.VMEM((unroll, 2 * ROWS, FIELDS), BF16),
            pltpu.SMEM((spheres + 8, ROWS), F32),
            pltpu.SemaphoreType.DMA((4, spheres)),
            pltpu.SemaphoreType.DMA,
        ],
        out_shape=[struct((2, ROWS, FIELDS)), struct((16, 64, LANES))],
        compiler_params=pltpu.CompilerParams(vmem_limit_bytes=52 * 1024 * 1024),
        cost_estimate=pl.CostEstimate(
            flops=6_000_000_000, bytes_accessed=10_000_000, transcendentals=0
        ),
        name="move",
    )(core, coefficients, shift_tables, weights)


def plane_kernel(got_ref, out_ref):
    total = got_ref[0]
    for k in range(1, 16):
        total = total + got_ref[k]
    group = lax.broadcasted_iota(jnp.int32, (8, LANES), 1) // CHUNK
    detectors = got_ref[3, 56:]
    for x in range(3):
        detectors = jnp.where(
            group == x, pltpu.roll(got_ref[x, 56:], (x + 1) * CHUNK, 1), detectors
        )
    for k in range(8):
        out_ref[k, :64] = total
        out_ref[k, 64:] = detectors


def tables_kernel(
    place_ref, const_ref, high_ref, low_ref, turned_ref, fixed_ref, gap_ref, waves_ref, phase_ref
):
    z, core = place_ref[0], place_ref[1]
    row = lambda shape: lax.broadcasted_iota(jnp.int32, shape, 0)
    step = math.pi / POLAR

    near = row((16, LANES))
    near = ((near // 4) * 8 + z) * 4 + near % 4
    plus, minus, _ = radial(const_ref, (near.astype(F32) + 0.5) * step)
    azim = row((32, LANES))
    azim = ((azim // 8) * 2 + core) * 8 + azim % 8
    turn = (azim * const_ref[0:1].astype(jnp.int32)) & (AZIM - 1)
    angle = turn.astype(F32) * (2.0 * math.pi / AZIM)
    for sign, table in enumerate((plus, minus)):
        for trig, wave in enumerate((jnp.cos(angle), jnp.sin(angle))):
            block = table[None, :, None, :] * wave.reshape(4, 1, 8, LANES)
            high, low = halves(block.reshape(2 * ROWS, LANES))
            lanes = slice((2 * sign + trig) * LANES, (2 * sign + trig + 1) * LANES)
            high_ref[:, lanes] = high
            low_ref[:, lanes] = low

    plus, minus, sine_theta = radial(
        const_ref, (row((POLAR, LANES)).astype(F32) + 0.5) * step
    )
    weight = sine_theta * (2.0 * math.pi * math.pi / (POLAR * AZIM))
    for sign, table in enumerate((plus, minus)):
        turned_ref[sign] = (table * weight).T
        high, low = halves(table)
        for block in range(2):
            fixed_ref[sign, block * LANES : (block + 1) * LANES, :LANES] = high
            fixed_ref[sign, block * LANES : (block + 1) * LANES, LANES:] = low

    across = lambda r: jnp.broadcast_to(const_ref[r : r + 1], (LANES, LANES))
    used = across(1) > 0
    order = across(0)
    gap = jnp.where(used, order, 200.0) - jnp.where(used, order, 100.0).T
    gap_ref[...] = gap
    phase_ref[0] = across(4).T
    phase_ref[1] = across(5).T

    shape = (LANES, LANES)
    lane = lax.broadcasted_iota(jnp.int32, shape, 1)
    for half in range(2):
        azim = row(shape) % CHUNK + half * CHUNK
        turn = (azim * (lane % 64) - jnp.where(lane < 64, 0, AZIM // 4)) & (AZIM - 1)
        wave = jnp.cos(turn.astype(F32) * (2.0 * math.pi / AZIM))
        waves_ref[:, half * LANES : (half + 1) * LANES] = wave


def power_kernel(turned_ref, fixed_ref, line_ref, waves_ref, gap_ref, out_ref):
    gap = gap_ref[...]
    detectors = line_ref[:, 64:].reshape(64, LANES)
    group = lax.broadcasted_iota(jnp.int32, detectors.shape, 1) // CHUNK
    detectors = jnp.concatenate([jnp.where(group == x, detectors, 0.0) for x in range(4)], axis=0)
    spectrum = jnp.dot(
        detectors, waves_ref[...], preferred_element_type=F32, precision=lax.Precision.HIGHEST
    )
    spectrum = spectrum[:, :LANES] + pltpu.roll(spectrum[:, LANES:], 2 * LANES - 4, 0)
    spectrum = jnp.concatenate([spectrum[8 * k : 8 * k + 4] for k in range(32)], axis=0)
    spectrum = spectrum.T
    far = jnp.abs(gap[:HALF])
    for sign in range(2):
        table = turned_ref[sign, :HALF]
        fixed = fixed_ref[sign]
        even = jnp.zeros((HALF, LANES), F32)
        odd = jnp.zeros((HALF, LANES), F32)
        for start in range(0, 2 * ORDER + 1, 7):
            rows, lows = [], []
            for d in range(start, start + 7):
                low = ((d - ORDER) ** 2 - 1) // 8 * 8 if d > ORDER else 0
                lows.append(low)
                rows += [table[low:] * spectrum[d : d + 1], table[low:] * spectrum[64 + d : 65 + d]]
            high, small = halves(jnp.concatenate(rows, axis=0))
            product = jnp.dot(
                jnp.concatenate([high, small], axis=1), fixed, preferred_element_type=F32
            )
            product = product[:, :LANES] + product[:, LANES:]
            at = 0
            for k, low in enumerate(lows):
                here, size = far[low:] == start + k, HALF - low
                new_even = jnp.where(here, product[at : at + size], even[low:])
                new_odd = jnp.where(here, product[at + size : at + 2 * size], odd[low:])
                at += 2 * size
                even = jnp.concatenate([even[:low], new_even], axis=0) if low else new_even
                odd = jnp.concatenate([odd[:low], new_odd], axis=0) if low else new_odd
        out_ref[sign, 0, :HALF] = even
        out_ref[sign, 1, :HALF] = jnp.where(gap[:HALF] < 0, -odd, odd)
        out_ref[sign, :, HALF:] = jnp.zeros((2, 8, LANES), F32)


def spread_rows(packed):
    parts = [packed] + [pltpu.roll(packed, LANES - g * CHUNK, 1) for g in (1, 2, 3)]
    return jnp.concatenate(parts, axis=0)


def columns(group, pieces):
    out = pieces[0]
    for g in (1, 2, 3):
        out = jnp.where(group == g, pltpu.roll(pieces[g], g * CHUNK, 1), out)
    return out


def far_kernel(
    core_ref, own_ref, other_ref, high_ref, low_ref, form_ref, phase_ref,
    incident_ref, incident_imag_ref, out_ref,
):
    core = core_ref[0]
    own, other = own_ref[...], other_ref[...]
    real = spread_rows(jnp.where(core == 0, own, other))
    imag = spread_rows(jnp.where(core == 0, other, own))
    group = lax.broadcasted_iota(jnp.int32, (HALF, LANES), 1) // CHUNK
    spare = jnp.zeros((8, LANES), F32)
    phase_real, phase_imag = phase_ref[0, :HALF], phase_ref[1, :HALF]
    real_1, real_2 = real[:HALF], real[HALF:COEFS]
    imag_1, imag_2 = imag[:HALF], imag[HALF:COEFS]
    rows = []
    collected = jnp.zeros((1, LANES), F32)
    for sign in range(2):
        if sign == 0:
            both = (real_2 - imag_1, imag_2 + real_1)
        else:
            both = (real_2 + imag_1, imag_2 - real_1)
        re = phase_real * both[0] - phase_imag * both[1]
        im = phase_real * both[1] + phase_imag * both[0]
        if sign == 0:
            top = columns(group, (re, im, -im, re))
            low = columns(group, (-im, re, -re, -im))
        else:
            top = columns(group, (re, im, im, -re))
            low = columns(group, (-im, re, re, im))
        rows += [0.5 * top, spare, 0.5 * low, spare]
        pair = jnp.concatenate([jnp.where(group == 0, re, 0.0), spare], axis=0)
        pair_imag = jnp.concatenate([jnp.where(group == 0, im, 0.0), spare], axis=0)
        dot = functools.partial(
            jnp.dot, preferred_element_type=F32, precision=lax.Precision.HIGHEST
        )
        even, odd = form_ref[sign, 0], form_ref[sign, 1]
        collected += 0.5 * jnp.sum(
            pair * dot(even, pair)
            + pair_imag * (dot(even, pair_imag) + 2.0 * dot(odd, pair)),
            axis=0,
            keepdims=True,
        )
    high, low = halves(jnp.concatenate(rows, axis=0))
    wide = jnp.dot(
        high_ref[...], jnp.concatenate([high, low], axis=1), preferred_element_type=F32
    )
    result = (
        wide[:, :LANES]
        + wide[:, LANES:]
        + jnp.dot(low_ref[...], high, preferred_element_type=F32)
    )
    extinction = jnp.sum(
        incident_ref[...] * real[:COEFS, :CHUNK] + incident_imag_ref[...] * imag[:COEFS, :CHUNK],
        axis=0,
        keepdims=True,
    )
    stats = jnp.concatenate(
        [
            extinction,
            real[COEFS : COEFS + 1, :CHUNK],
            collected[:, :CHUNK],
            jnp.zeros((1, CHUNK), F32),
        ],
        axis=1,
    )
    stats = jnp.broadcast_to(stats, (8, LANES))
    for k in range(16):
        out_ref[k, :CHUNK] = result[k * CHUNK : (k + 1) * CHUNK]
        out_ref[k, CHUNK:] = stats


def finish_kernel(place_ref, got_ref, amplitude_ref, stats_ref):
    for tile in range(4):
        blocks = [got_ref[4 * tile + x, :CHUNK] for x in range(4)]
        for q, block in enumerate(swap_chunks(blocks)):
            amplitude_ref[q, :, tile * LANES : (tile + 1) * LANES] = block
    place = place_ref[0]
    first = got_ref[place, CHUNK : CHUNK + 1]
    second = got_ref[place + 1, CHUNK : CHUNK + 1]
    stats_ref[...] = jnp.concatenate(
        [
            jnp.concatenate(
                [v[:, r * CHUNK : (r + 1) * CHUNK] for v in (first, second)], axis=1
            )
            for r in range(3)
        ],
        axis=0,
    )


def shards(coefficients, positions, shift_tables, absorb_weight, incident, detector):
    x, z = lax.axis_index("sph_0"), lax.axis_index("sph_1")
    y, core = lax.axis_index("ang_0"), lax.axis_index("ang_1")
    smem = pl.BlockSpec(memory_space=pltpu.SMEM)
    vmem = pl.BlockSpec(memory_space=pltpu.VMEM)

    total, theirs = moved_sum(
        coefficients, positions, shift_tables, absorb_weight, core.reshape(1)
    )
    other = lax.ppermute(theirs, PAIR, [(0, 1), (1, 0)])
    (mine,) = call(
        pack_kernel,
        [struct((16, 64, LANES))],
        [core.reshape(1), total, detector],
        flops=10_000_000,
        in_specs=[smem, vmem, vmem],
    )
    packed = mine + other
    packed, incident, x, z, y, core = lax.optimization_barrier(
        (packed, incident, x, z, y, core)
    )
    high, low, turned, fixed, gap, waves, phase = call(
        tables_kernel,
        [
            struct((2 * ROWS, 2 * ROWS), BF16), struct((2 * ROWS, 2 * ROWS), BF16),
            struct((2, LANES, POLAR)), struct((2, 2 * POLAR, 2 * LANES), BF16), struct((LANES, LANES)),
            struct((LANES, 2 * LANES)), struct((2, LANES, LANES)),
        ],
        [jnp.stack([z, core]), jnp.asarray(constants())],
        flops=100_000_000,
        in_specs=[smem, vmem],
    )
    first = (4 * y + x) * CHUNK
    tables = (
        turned, fixed, waves, gap, high, low, phase,
        lax.dynamic_slice_in_dim(incident, first, CHUNK, 1),
        lax.dynamic_slice_in_dim(incident, FIELDS + first, CHUNK, 1),
        core.astype(jnp.int32).reshape(1), (4 * y + 2 * core).astype(jnp.int32).reshape(1),
    )
    got = lax.all_to_all(packed, PLANE, 0, 0, tiled=True)
    got, tables = lax.optimization_barrier((got, tables))
    turned, fixed, waves, gap, high, low, phase, inc_real, inc_imag, core, place = tables
    (spread,) = call(plane_kernel, [struct((8, 72, LANES))], [got])
    line = lax.all_to_all(spread, LINE, 0, 0, tiled=True)
    own = line[:, :64].sum(axis=0)
    partner = lax.ppermute(own, PAIR, [(0, 1), (1, 0)])
    (form,) = call(
        power_kernel,
        [struct((2, 2, LANES, LANES))],
        [turned, fixed, line, waves, gap],
        flops=1_000_000_000,
    )
    (messages,) = call(
        far_kernel,
        [struct((16, 40, LANES))],
        [core, own, partner, high, low, form, phase, inc_real, inc_imag],
        flops=400_000_000,
        in_specs=[smem] + [vmem] * 8,
    )
    got = lax.all_to_all(messages, PLANE, 0, 0, tiled=True)
    amplitude, stats = call(
        finish_kernel,
        [struct((4, 32, FIELDS)), struct((3, 64))],
        [place, got],
        in_specs=[smem, vmem],
    )
    return (amplitude.reshape(2, 2, 4, 8, FIELDS), stats)


def solution(mesh):
    torus = Mesh(mesh.devices.reshape(4, 8, 4, 2), SPH_ANG)
    in_specs = (P(SPH_ANG, None, None), P(SPH_ANG, None), P(), P(SPH_ANG, None), P(), P(SPH, None))
    out_specs = (P(None, None, SPH, ANG, None), P(None, ANG))
    return jax.shard_map(
        shards, mesh=torus, in_specs=in_specs, out_specs=out_specs, check_vma=False
    )
```
